128 devices in a mesh: col: 64 (over y_lo, z, x, core), row: 2 (over y_hi).
Axes of the slice: x: 4, y: 4 (y_hi: 2, y_lo: 2; y = y_hi * 2 + y_lo), z: 4, core: 2. Of those that a mesh axis runs over, the one named last changes fastest.
Arguments:
- matrix: float32 [8192, 8192], P('row', 'col'), as said below
- row_diag: float32 [2, 8192], P(None, 'row'), may hold values from 0.8 to 1.2
- col_diag: float32 [2, 8192], P(None, 'col'), may hold values from 0.8 to 1.2
Outputs:
- factored: float32 [8192, 8192], P('row', 'col')
The draws below stay inside these ranges and needn't reach their ends.
Inputs may be any that keep to these rules, and one draw needn't show every extreme that they name: `matrix`: off the diagonal the entries lie within -6 and 6; the diagonal entries exceed 1.5 * sqrt(512) - 6.
All inputs are finite; a program needn't handle non-finite values.
Results may differ from the reference program's by a relative error of at most 0.0001.
Values sent between devices are 32-bit elements; how exact they have to be, the bound alone decides.
A program may use at most 64 MiB of HBM per device.

```python
import jax
import jax.numpy as jnp
from jax import lax

PW = 256
PANELS = 2
NORD = 8192


def draw_matrix(key, part):
    noise_key = jax.random.fold_in(key, 11)
    diag_key = jax.random.fold_in(key, 23)
    noise = jnp.clip(jax.random.normal(noise_key, (NORD, NORD), jnp.float32), -6.0, 6.0)
    leading = jax.random.uniform(diag_key, (NORD,), jnp.float32, 1.5, 2.5) * jnp.sqrt(jnp.float32(PANELS * PW))
    return noise + jnp.diag(leading)


def setup_inputs(seed: int = 0) -> dict:
    key_list = jax.random.split(jax.random.key(seed), 4)
    matrix = draw_matrix(jax.random.fold_in(key_list[3], 71), 0)
    row_diag = jnp.clip(1.0 + 0.04 * jax.random.normal(key_list[1], (2, NORD), jnp.float32), 0.8, 1.2)
    col_diag = jnp.clip(1.0 + 0.04 * jax.random.normal(key_list[2], (2, NORD), jnp.float32), 0.8, 1.2)
    return {"matrix": matrix, "row_diag": row_diag, "col_diag": col_diag}


inv_root = 0.7071067811865476


def mix_halves(values, scales, axis):
    half = values.shape[axis] // 2
    if axis == 0:
        upper_part, lower_part = values[:half], values[half:]
        first, second = scales[:half, None], scales[half:, None]
    else:
        upper_part, lower_part = values[:, :half], values[:, half:]
        first, second = scales[None, :half], scales[None, half:]
    return jnp.concatenate([first * (upper_part + lower_part) * inv_root, second * (upper_part - lower_part) * inv_root], axis)


def level_two(values, scales, axis):
    half = values.shape[axis] // 2
    if axis == 0:
        left_part, right_part = values[:half], values[half:]
    else:
        left_part, right_part = values[:, :half], values[:, half:]
    return jnp.concatenate([mix_halves(left_part, scales[:half], axis), mix_halves(right_part, scales[half:], axis)], axis)


def lu_block(block):
    size = block.shape[0]
    places = jnp.arange(size)

    def eliminate(step, current):
        pivot = current[step, step]
        below = places > step
        column = jnp.where(below, current[:, step] / pivot, 0.0)
        across = jnp.where(below, current[step, :], 0.0)
        current = current - column[:, None] * across[None, :]
        return jnp.where((places == step)[None, :] & below[:, None], column[:, None], current)

    return lax.fori_loop(0, size, eliminate, block)


def hdot(left, right):
    return jnp.dot(left, right, precision=lax.Precision.HIGHEST, preferred_element_type=jnp.float32)


def strict_inverse(strict):
    size = strict.shape[0]
    identity = jnp.eye(size, dtype=strict.dtype)
    result = identity - strict
    power = strict
    exponent = 1
    while exponent * 2 < size:
        power = hdot(power, power)
        exponent = exponent * 2
        result = hdot(result, identity + power)
    return result


def inverses(packed):
    upper_factor = jnp.triu(packed)
    lower_inverse = strict_inverse(jnp.tril(packed, -1))
    pivots = jnp.diagonal(packed)
    scaled = jnp.triu(packed, 1) / pivots[:, None]
    upper_inverse = strict_inverse(scaled) / pivots[None, :]
    return lower_inverse, upper_inverse, upper_factor


def reference(matrix, row_diag, col_diag):
    current = mix_halves(matrix, row_diag[0], 0)
    current = level_two(current, row_diag[1], 0)
    current = mix_halves(current, col_diag[0], 1)
    current = level_two(current, col_diag[1], 1)
    for panel in range(PANELS):
        start = panel * PW
        stop = start + PW
        packed = lu_block(current[start:stop, start:stop])
        lower_inverse, upper_inverse, upper_factor = inverses(packed)
        lower_rows = hdot(current[stop:, start:stop], upper_inverse)
        upper_cols = hdot(lower_inverse, current[start:stop, stop:])
        trailing = current[stop:, stop:] - hdot(lower_rows, upper_cols)
        current = current.at[start:stop, start:stop].set(packed)
        current = current.at[stop:, start:stop].set(lower_rows)
        current = current.at[start:stop, stop:].set(upper_cols)
        current = current.at[stop:, stop:].set(trailing)
    return current
```

```python
import jax
import jax.numpy as jnp
from jax import lax
from jax.experimental import pallas as pl
from jax.experimental.pallas import tpu as pltpu
from jax.sharding import PartitionSpec as P

HI = lax.Precision.HIGHEST


def hdot(a, b):
    return jnp.dot(a, b, precision=HI, preferred_element_type=jnp.float32)


def rows_to(x, height):
    return jnp.broadcast_to(x, (height, x.shape[1]))


def lane_to(x, lane, width=128):
    return jnp.broadcast_to(x[:, lane : lane + 1], (x.shape[0], width))


def lu128(s, group=4):
    sub = lax.broadcasted_iota(jnp.int32, (8, 128), 0)
    lane = lax.broadcasted_iota(jnp.int32, (8, 128), 1)
    tiles = [s[8 * t : 8 * t + 8, :] for t in range(16)]
    extra = [jnp.where(lane == sub + 8 * t, 1.0, 0.0) for t in range(16)]
    packed = [None] * 16
    for b in range(16):
        rows, rows2 = tiles[b], extra[b]
        cols = [lane_to(rows, 8 * b + c) for c in range(8)]
        inv, ups, u = [], [], {}
        for c in range(8):
            r = 1.0 / rows_to(cols[c][c : c + 1], 8)
            inv.append(r)
            m = jnp.where(sub > c, cols[c] * r, 0.0)
            top = jnp.where(lane > 8 * b + c, rows_to(rows[c : c + 1], 8), 0.0)
            rows = jnp.where((lane == 8 * b + c) & (sub > c), m, rows - m * top)
            if c < 7:
                rows2 = rows2 - m * rows_to(rows2[c : c + 1], 8)
            for d in range(c + 1, 8):
                u[c, d] = rows_to(cols[d][c : c + 1], 8)
                cols[d] = cols[d] - m * u[c, d]
        packed[b] = rows
        extra[b] = rows2
        inside = (lane >= 8 * b) & (lane < 8 * b + 8)
        past = lane >= 8 * b + 8
        tiles[b] = jnp.where(lane == sub + 8 * b, 1.0, 0.0)
        ups = []
        for c in range(8):
            top = jnp.where(past, rows_to(rows[c : c + 1], 8), 0.0)
            ups.append(jnp.where(lane == 8 * b + c, -1.0, top))
        ups2 = [rows_to(rows2[c : c + 1], 8) for c in range(8)]
        order = list(range(b + 1, 16)) + list(range(b + 1))
        for t in order:
            tile = tiles[t]
            ls = [lane_to(tile, 8 * b + c) for c in range(8)]
            for c in range(8):
                ls[c] = ls[c] * inv[c]
                for d in range(c + 1, 8):
                    ls[d] = ls[d] - ls[c] * u[c, d]
            tile = jnp.where(inside, 0.0, tile)
            for c in range(8):
                tile = tile - ls[c] * ups[c]
            tiles[t] = tile
            if t > b:
                e = extra[t]
                for c in range(8):
                    e = e - ls[c] * ups2[c]
                extra[t] = e
    return packed, extra, tiles


def lu_kernel(a_ref, p_ref, li_ref, ui_ref):
    n = a_ref.shape[0]
    nb = n // 128
    ui_ref[...] = a_ref[...]
    ri = lax.broadcasted_iota(jnp.int32, (n, n), 0)
    ci = lax.broadcasted_iota(jnp.int32, (n, n), 1)
    li_ref[...] = jnp.where(ri == ci, 1.0, 0.0)

    def step(k, _):
        o = pl.multiple_of(k * 128, 128)
        blk = pl.ds(o, 128)
        packed, lower, upper = lu128(ui_ref[blk, blk])
        packed = jnp.concatenate(packed, 0)
        lower = jnp.concatenate(lower, 0)
        upper = jnp.concatenate(upper, 0)
        bc = lax.broadcasted_iota(jnp.int32, (128, n), 1)
        br = lax.broadcasted_iota(jnp.int32, (128, n), 0)
        band = ui_ref[blk, :]
        right = hdot(lower, band)
        p_ref[blk, :] = jnp.where(bc >= o + 128, right, band)
        p_ref[blk, blk] = packed
        right = jnp.where(bc >= o + 128, right, 0.0)
        ui_ref[blk, :] = jnp.where(bc == br + o, 1.0, 0.0)
        lband = hdot(lower, li_ref[blk, :])
        li_ref[blk, :] = lband
        left = hdot(ui_ref[:, blk], upper)
        ui_ref[...] = ui_ref[...] - hdot(left, right)
        ui_ref[:, blk] = left
        lr = lax.broadcasted_iota(jnp.int32, (n, 128), 0)
        li_ref[...] = li_ref[...] - hdot(jnp.where(lr >= o + 128, left, 0.0), lband)
        return 0

    lax.fori_loop(0, nb, step, 0)


MESH = pl.DeviceIdType.MESH
VMEM = pl.BlockSpec(memory_space=pltpu.VMEM)
inv_root = 0.7071067811865476


def place():
    r, c = lax.axis_index("row"), lax.axis_index("col")
    return r * 4 + c // 16, c % 16


def member(m, g):
    return {"row": m // 4, "col": (m % 4) * 16 + g}


def remote(src, dst, send, recv, device):
    return pltpu.make_async_remote_copy(
        src, dst, send, recv, device_id=device, device_id_type=MESH
    )


def a2a_kernel(x_ref, o_ref, send, recv):
    m, g = place()
    bar = pltpu.get_barrier_semaphore()
    for d in range(1, 8):
        pl.semaphore_signal(bar, inc=1, device_id=member((m + d) % 8, g), device_id_type=MESH)
    pl.semaphore_wait(bar, 7)
    copies = []
    for d in range(1, 8):
        p = (m + d) % 8
        copies.append(remote(x_ref.at[p], o_ref.at[m], send.at[d], recv.at[d], member(p, g)))
        copies[-1].start()
    o_ref[m] = x_ref[m]
    for copy in copies:
        copy.wait()


def a2a(x, cid):
    return pl.pallas_call(
        a2a_kernel,
        out_shape=jax.ShapeDtypeStruct(x.shape, x.dtype),
        in_specs=[VMEM],
        out_specs=VMEM,
        scratch_shapes=[pltpu.SemaphoreType.DMA((8,)), pltpu.SemaphoreType.DMA((8,))],
        compiler_params=pltpu.CompilerParams(collective_id=cid, has_side_effects=True),
        name="a2a%d" % cid,
    )(x)


def gather_kernel(x_ref, b_ref, m11_ref, m12_ref, m21_ref, s0, r0, s1, r1, s2, r2, s3, r3, s4, r4):
    m, g = place()
    bar = pltpu.get_barrier_semaphore()
    for d in range(1, 8):
        pl.semaphore_signal(bar, inc=1, device_id=member((m + d) % 8, g), device_id_type=MESH)
    for d in range(1, 16):
        pl.semaphore_signal(bar, inc=1, device_id=member(m, (g + d) % 16), device_id_type=MESH)
    pl.semaphore_wait(bar, 22)

    def top(d):
        return remote(x_ref.at[0], m21_ref.at[0, g], s0.at[d], r0.at[g], member(m, (g + d) % 16))

    def part(d):
        p = (g + d) % 16
        return remote(x_ref.at[p], m21_ref.at[p, g], s1.at[d], r1.at[g], member(m, p))

    @pl.when(g < 4)
    def _():
        for d in range(1, 16):
            top(d).start()
        for d in range(1, 16):

            @pl.when((g + d) % 16 != 0)
            def _():
                part(d).start()

        m21_ref[0, g] = x_ref[0]
        m21_ref[g, g] = x_ref[g]

    bands = [
        remote(b_ref, m12_ref.at[m], s2.at[d], r2.at[d], member((m + d) % 8, g))
        for d in range(1, 8)
    ]
    for copy in bands:
        copy.start()
    m12_ref[m] = b_ref[...]
    for s in range(4):

        @pl.when(g != s)
        def _():
            remote(x_ref.at[0], m21_ref.at[0, s], s0.at[0], r0.at[s], member(m, (g + 1) % 16)).wait_recv()

    corners = [
        remote(m21_ref.at[0], m11_ref.at[m], s3.at[d], r3.at[d], member((m + d) % 8, g))
        for d in range(1, 8)
    ]
    for copy in corners:
        copy.start()
    m11_ref[m] = m21_ref[0]

    @pl.when(g != 0)
    def _():
        for s in range(4):

            @pl.when(g != s)
            def _():
                remote(x_ref.at[0], m21_ref.at[g, s], s1.at[0], r1.at[s], member(m, (g + 1) % 16)).wait_recv()

        for d in range(1, 16):
            remote(m21_ref.at[g], m21_ref.at[g], s4.at[d], r4.at[g], member(m, (g + d) % 16)).start()

    for p in range(1, 16):

        @pl.when(g != p)
        def _():
            remote(m21_ref.at[g], m21_ref.at[p], s4.at[0], r4.at[p], member(m, (g + 1) % 16)).wait_recv()

    for copy in corners + bands:
        copy.wait()

    @pl.when(g < 4)
    def _():
        for d in range(1, 16):
            top(d).wait_send()
        for d in range(1, 16):

            @pl.when((g + d) % 16 != 0)
            def _():
                part(d).wait_send()

    @pl.when(g != 0)
    def _():
        for d in range(1, 16):
            remote(m21_ref.at[g], m21_ref.at[g], s4.at[d], r4.at[g], member(m, (g + d) % 16)).wait_send()


def gather(x, b):
    shapes = [(8, 4, 64, 128), (8, 64, 512), (16, 4, 64, 128)]
    counts = [16, 4, 16, 4, 8, 8, 8, 8, 16, 16]
    return pl.pallas_call(
        gather_kernel,
        out_shape=[jax.ShapeDtypeStruct(s, jnp.float32) for s in shapes],
        in_specs=[VMEM] * 2,
        out_specs=[VMEM] * 3,
        scratch_shapes=[pltpu.SemaphoreType.DMA((n,)) for n in counts],
        compiler_params=pltpu.CompilerParams(collective_id=2, has_side_effects=True),
        name="gather",
    )(x, b)


def lu(a):
    n = a.shape[0]
    return pl.pallas_call(
        lu_kernel,
        out_shape=[jax.ShapeDtypeStruct((n, n), jnp.float32)] * 3,
        in_specs=[VMEM],
        out_specs=[VMEM] * 3,
        cost_estimate=pl.CostEstimate(
            flops=40_000_000_000, bytes_accessed=4 << 20, transcendentals=0
        ),
        name="lu",
    )(a)


def spread(x):
    rest = x.shape[1:]
    return jnp.concatenate(
        [x[:512].reshape(8, 64, *rest), x[512:].reshape(8, 192, *rest)], 1
    )


def unspread(x):
    rest = x.shape[2:]
    return jnp.concatenate(
        [x[:, :64].reshape(512, *rest), x[:, 64:].reshape(1536, *rest)], 0
    )


def mixed(x, axis, scale):
    first, second = lax.index_in_dim(x, 0, axis), lax.index_in_dim(x, 1, axis)
    return scale * jnp.concatenate([first + second, first - second], axis) * inv_root


def shards(matrix, row_diag, col_diag):
    m, g = place()
    halves = jnp.stack([spread(matrix[:2048]), spread(matrix[2048:])], 1)
    scales = jnp.stack(
        [jnp.stack([spread(row_diag[l][:2048]), spread(row_diag[l][2048:])], 1) for l in range(2)], 1
    )
    scales = scales.reshape(8, 8, 128)
    across = jnp.broadcast_to(jnp.pad(col_diag, ((0, 6), (0, 0)))[None], (8, 8, 128))
    got = a2a(jnp.concatenate([halves.reshape(8, 512, 128), scales, across], 1), 0)
    body = got[:, :512].reshape(2, 2, 2, 2, 256, 128)
    rd = got[:, 512:520].reshape(2, 4, 2, 2, 256)[:, 0]
    cd = got[:4, 520:522]
    body = mixed(body, 0, rd[:, 0][:, None, None, :, :, None])
    body = mixed(body, 3, rd[:, 1][:, None, None, :, :, None])
    body = mixed(body, 1, cd[:, 0].reshape(1, 2, 2, 1, 1, 128))
    body = mixed(body, 2, cd[:, 1].reshape(1, 2, 2, 1, 1, 128))
    body = body.reshape(2, 4, 512, 128)
    flat = body.transpose(0, 2, 1, 3).reshape(1024, 512)
    corner, band, panel = gather(flat[:, :128].reshape(16, 64, 128), flat[:64])
    corner = corner.transpose(0, 2, 1, 3).reshape(512, 512)
    band = band.reshape(512, 512)
    panel = panel.transpose(0, 2, 1, 3).reshape(1024, 512)
    packed, lower, upper = lu(corner)
    right = hdot(lower, band)
    left = jnp.dot(panel, upper, precision=lax.Precision.HIGH, preferred_element_type=jnp.float32)
    rest = flat - jnp.dot(left, right, precision=lax.Precision.HIGH, preferred_element_type=jnp.float32)
    own = jnp.clip(g, 0, 3) * 128
    first = jnp.where(g < 4, lax.dynamic_slice_in_dim(left, own, 128, 1), rest[:, :128])
    top = lax.dynamic_slice_in_dim(right, 64 * m, 64, 0)
    corner_own = lax.dynamic_slice(packed, (64 * m, own), (64, 128))
    top_first = jnp.where(g < 4, corner_own, top[:, :128])
    done = jnp.concatenate(
        [
            jnp.concatenate([top_first, top[:, 128:]], 1),
            jnp.concatenate([first[64:], rest[64:, 128:]], 1),
        ],
        0,
    )
    back = a2a(done.reshape(2, 512, 4, 128).transpose(0, 2, 1, 3).reshape(8, 512, 128), 1)
    back = back.reshape(8, 2, 256, 128)
    return jnp.concatenate([unspread(back[:, 0]), unspread(back[:, 1])], 0)


def solution(mesh):
    in_specs = (P("row", "col"), P(None, "row"), P(None, "col"))
    out_specs = P("row", "col")
    return jax.shard_map(shards, mesh=mesh, in_specs=in_specs, out_specs=out_specs, check_vma=False)
```

```python
import jax
import jax.numpy as jnp
from jax import lax
from jax.experimental import pallas as pl
from jax.experimental.pallas import tpu as pltpu
from jax.sharding import PartitionSpec as P

MESH = pl.DeviceIdType.MESH
VMEM = pl.BlockSpec(memory_space=pltpu.VMEM)
GROUP = 4


def split(a):
    high = a.astype(jnp.bfloat16)
    return high, (a - high.astype(jnp.float32)).astype(jnp.bfloat16)


def dot(a, b):
    return jnp.dot(a, b, preferred_element_type=jnp.float32)


def dot3(a, b):
    return dot(a[0], b[0]) + (dot(a[0], b[1]) + dot(a[1], b[0]))


def rows_to(x, height):
    return jnp.broadcast_to(x, (height, x.shape[1]))


def lane_to(x, lane):
    return jnp.broadcast_to(x[:, lane : lane + 1], (x.shape[0], 128))


def lu128(s):
    height = 8 * GROUP
    sub = lax.broadcasted_iota(jnp.int32, (8, 128), 0)
    lane = lax.broadcasted_iota(jnp.int32, (8, 128), 1)
    subs = lax.broadcasted_iota(jnp.int32, (height, 128), 0)
    lanes = lax.broadcasted_iota(jnp.int32, (height, 128), 1)
    count = 16 // GROUP
    tiles = [s[height * t : height * t + height] for t in range(count)]
    extra = [jnp.where(lanes == subs + height * t, 1.0, 0.0) for t in range(count)]
    packed, lower = [], []

    def tall(x):
        return jnp.concatenate([x] * GROUP, 0)

    for b in range(16):
        at, part = b // GROUP, 8 * (b % GROUP)
        rows, rows2 = tiles[at][part : part + 8], extra[at][part : part + 8]
        cols = [lane_to(rows, 8 * b + c) for c in range(8)]
        inv, u = [], {}
        for c in range(8):
            r = 1.0 / rows_to(cols[c][c : c + 1], 8)
            inv.append(tall(r))
            factor = jnp.where(sub > c, cols[c] * r, 0.0)
            top = jnp.where(lane > 8 * b + c, rows_to(rows[c : c + 1], 8), 0.0)
            rows = jnp.where((lane == 8 * b + c) & (sub > c), factor, rows - factor * top)
            if c < 7:
                rows2 = rows2 - factor * rows_to(rows2[c : c + 1], 8)
            for d in range(c + 1, 8):
                row = rows_to(cols[d][c : c + 1], 8)
                u[c, d] = tall(row)
                cols[d] = cols[d] - factor * row
        packed.append(rows)
        lower.append(rows2)
        pieces = [jnp.where(lane == sub + 8 * b, 1.0, 0.0)]
        if part:
            pieces = [tiles[at][:part]] + pieces
        if part + 8 < height:
            pieces = pieces + [tiles[at][part + 8 :]]
        tiles[at] = jnp.concatenate(pieces, 0) if len(pieces) > 1 else pieces[0]
        inside = (lanes >= 8 * b) & (lanes < 8 * b + 8)
        ups, ups2 = [], []
        for c in range(8):
            top = jnp.where(lane >= 8 * b + 8, rows_to(rows[c : c + 1], 8), 0.0)
            ups.append(tall(jnp.where(lane == 8 * b + c, -1.0, top)))
            ups2.append(tall(rows_to(rows2[c : c + 1], 8)))
        for i in range(count):
            t = ((b + 1) // GROUP + i) % count
            tile = tiles[t]
            ls = [lane_to(tile, 8 * b + c) for c in range(8)]
            for c in range(8):
                ls[c] = ls[c] * inv[c]
                for d in range(c + 1, 8):
                    ls[d] = ls[d] - ls[c] * u[c, d]
            tile = jnp.where(inside, 0.0, tile)
            for c in range(8):
                tile = tile - ls[c] * ups[c]
            tiles[t] = tile
            if (t + 1) * GROUP - 1 > b:
                tile = extra[t]
                for c in range(8):
                    tile = tile - ls[c] * ups2[c]
                extra[t] = tile
    return tuple(jnp.concatenate(x, 0) for x in (packed, lower, tiles))


def lu_step(k, packed, li, ui):
    n = ui.shape[0]
    o = pl.multiple_of(k * 128, 128)
    blk = pl.ds(o, 128)
    own, lower, upper = lu128(ui[blk, blk])
    lower, upper = split(lower), split(upper)
    past = lax.broadcasted_iota(jnp.int32, (128, n), 1) >= o + 128
    diag = lax.broadcasted_iota(jnp.int32, (128, n), 1) == (
        lax.broadcasted_iota(jnp.int32, (128, n), 0) + o
    )
    band = ui[blk, :]
    right = dot3(lower, split(band))
    packed[blk, :] = jnp.where(past, right, band)
    packed[blk, blk] = own
    ui[blk, :] = jnp.where(diag, 1.0, 0.0)
    left = dot3(split(ui[:, blk]), upper)
    ui[...] = ui[...] - dot3(split(left), split(jnp.where(past, right, 0.0)))
    ui[:, blk] = left
    lband = dot3(lower, split(li[blk, :]))
    li[blk, :] = lband
    below = lax.broadcasted_iota(jnp.int32, (n, 128), 0) >= o + 128
    li[...] = li[...] - dot3(split(jnp.where(below, left, 0.0)), split(lband))


def kernel(x, s, o, xin, sin, rs, t, m11, m12, m21, packed, li, ui, lh, ll, lf, uf, uh, ul, z, send, recv):
    r, c = lax.axis_index("row"), lax.axis_index("col")
    m, g = r * 4 + c // 16, c % 16
    core, pair = g % 2, g // 2

    def member(p):
        return {"row": p // 4, "col": (p % 4) * 16 + g}

    def chip(d):
        return {"row": r, "col": (m % 4) * 16 + (g + 2 * d) % 16}

    partner = {"row": r, "col": (m % 4) * 16 + g + 1 - 2 * core}

    def device(p):
        return {"row": r, "col": (m % 4) * 16 + p}

    def remote(src, dst, kind, out, into, where):
        return pltpu.make_async_remote_copy(
            src, dst, send.at[kind, out], recv.at[kind, into], device_id=where, device_id_type=MESH
        )

    def rows(p, height, base=0):
        return pl.ds(pl.multiple_of(base + height * p, 8), height)

    def head(d):
        p = (m + d) % 8
        return remote(x.at[:, rows(p, 64)], xin.at[m, :, pl.ds(0, 64)], 0, d, d, member(p))

    def small(d):
        p = (m + d) % 8
        return remote(s.at[p], sin.at[m], 1, d, d, member(p))

    def tail(d, half):
        p = (m + d) % 8
        return remote(
            x.at[half, rows(p, 192, 512)], xin.at[m, half, pl.ds(64, 192)], 2 + half, d, d, member(p)
        )

    def top(d):
        return remote(t.at[0, 0, pl.ds(0, 64)], m21.at[0, core, pair], 4, d, pair, chip(d))

    def top_over():
        return remote(m21.at[0, core], m21.at[0, core], 5, 0, 0, partner)

    def corner(d):
        return remote(m21.at[0, core], m11.at[m, core], 6, d, d, member((m + d) % 8))

    def corner_over(d):
        p = (m + 8 - d) % 8
        return remote(m11.at[p, core], m11.at[p, core], 7, d, d, partner)

    def band(d):
        return remote(t.at[pl.ds(0, 4), 0, pl.ds(0, 64)], m12.at[m], 8, d, d, member((m + d) % 8))

    def piece(p):
        return t.at[(p // 8) * 4, (p % 8) // 4, rows(p % 4, 64)]

    def part(d):
        p = (g + d) % 16
        return remote(piece(p), m21.at[p, core, pair], 9, d, g, device(p))

    def panel(d):
        return remote(m21.at[g], m21.at[g], 10, d, pair, chip(d))

    def panel_over(j):
        p = 2 * j + core
        return remote(m21.at[p], m21.at[p], 11, j, j, partner)

    def back(d, first):
        p = (m + d) % 8
        if first:
            return remote(z.at[p, :, pl.ds(0, 64)], o.at[:, rows(m, 64)], 12, d, d, member(p))
        return remote(z.at[p, :, pl.ds(64, 192)], o.at[:, rows(m, 192, 512)], 13, d, d, member(p))

    bar = pltpu.get_barrier_semaphore()
    for d in range(1, 8):
        pl.semaphore_signal(bar, inc=1, device_id=member((m + d) % 8), device_id_type=MESH)
    for d in range(1, 16):
        pl.semaphore_signal(bar, inc=1, device_id=device((g + d) % 16), device_id_type=MESH)
    pl.semaphore_wait(bar, 22)

    for d in range(1, 8):
        small(d).start()
    for d in range(1, 8):
        head(d).start()
    sin[m] = s[m]
    xin[m, :, 0:64] = x[:, rows(m, 64)]
    xin[m, :, 64:256] = x[:, rows(m, 192, 512)]
    for d in range(1, 8):
        tail(d, 0).start()
    for d in range(1, 8):
        small(d).wait()
    for l in range(2):
        for i in range(2):
            for j in range(2):
                for h in range(2):
                    line = sin[4 * i, 4 * l + 2 * j + h : 4 * l + 2 * j + h + 1, :]
                    rs[l, i, j, 128 * h : 128 * h + 128] = rows_to(line, 128).T

    def mix(j, _):
        at = pl.ds(pl.multiple_of(8 * j, 8), 8)
        first = [rows_to(sin[q, 8:9, :], 8) for q in range(4)]
        second = [rows_to(sin[q, 9:10, :] * 0.25, 8) for q in range(4)]
        for i in range(2):
            mid = {}
            for q in range(4):
                y = []
                for h in range(2):
                    a, b = xin[q, h, at], xin[4 + q, h, at]
                    y.append(rs[0, i, h, at] * (a + b if i == 0 else a - b))
                mid[q] = [rs[1, i, 0, at] * (y[0] + y[1]), rs[1, i, 1, at] * (y[0] - y[1])]
            for h in range(2):
                w = [first[q] * (mid[q][h] + mid[q + 2][h]) for q in range(2)]
                w += [first[q + 2] * (mid[q][h] - mid[q + 2][h]) for q in range(2)]
                for q in (0, 2):
                    t[4 * i + q, h, at] = second[q] * (w[q] + w[q + 1])
                    t[4 * i + q + 1, h, at] = second[q + 1] * (w[q] - w[q + 1])
        return 0

    for d in range(1, 8):
        head(d).wait()
    lax.fori_loop(0, 8, mix, 0)

    @pl.when(g < 4)
    def _():
        for d in range(1, 8):
            top(d).start()
        m21[0, core, pair] = t[0, 0, 0:64]

    for i in range(2):

        @pl.when(g != 2 * i + core)
        def _():
            remote(t.at[0, 0, pl.ds(0, 64)], m21.at[0, core, i], 4, 0, i, partner).wait_recv()

    for d in range(1, 8):
        corner(d).start()
    top_over().start()
    for d in range(1, 8):
        tail(d, 1).start()
    for d in range(1, 8):
        band(d).start()
    m11[m, core] = m21[0, core]
    m12[m] = t[0:4, 0, 0:64]
    li[...] = jnp.where(
        lax.broadcasted_iota(jnp.int32, li.shape, 0) == lax.broadcasted_iota(jnp.int32, li.shape, 1),
        1.0,
        0.0,
    )
    top_over().wait()
    m11[m, 1 - core] = m21[0, 1 - core]
    for d in range(1, 8):
        corner(d).wait_recv()
        corner_over(d).start()
    for d in range(1, 8):
        corner_over(d).wait()
    for i in range(8):
        for j in range(4):
            ui[64 * i : 64 * i + 64, 128 * j : 128 * j + 128] = m11[i, j % 2, j // 2]

    def eliminate(k, _):
        lu_step(k, packed, li, ui)

        @pl.when(k == 0)
        def _():
            for d in range(1, 8):
                tail(d, 0).wait()
                tail(d, 1).wait()
            lax.fori_loop(8, 32, mix, 0)

            @pl.when(g < 4)
            def _():
                for d in range(1, 16):

                    @pl.when((g + d) % 16 != 0)
                    def _():
                        part(d).start()

                @pl.when(g != 0)
                def _():
                    m21[g, core, pair] = t[0, 0, rows(g, 64)]

        @pl.when(k == 1)
        def _():
            @pl.when(g != 0)
            def _():
                for i in range(4):

                    @pl.when(g != i)
                    def _():
                        remote(
                            piece(g), m21.at[g, i % 2, i // 2], 9, 0, i, partner
                        ).wait_recv()

                for d in range(1, 8):
                    panel(d).start()
                panel_over(pair).start()

        @pl.when(k == 2)
        def _():
            for j in range(8):

                @pl.when((2 * j + core != 0) & (j != pair))
                def _():
                    remote(m21.at[g], m21.at[2 * j + core], 10, 0, j, partner).wait_recv()
                    panel_over(j).start()

        return 0

    lax.fori_loop(0, 4, eliminate, 0)

    for d in range(1, 8):
        corner(d).wait_send()
        band(d).wait()
    lower = split(li[...])
    for q in range(4):
        lanes = slice(128 * q, 128 * q + 128)
        uf[:, lanes] = dot3(lower, split(m12[:, q].reshape(512, 128)))
        uh[:, lanes], ul[:, lanes] = split(uf[:, lanes])

    @pl.when(g < 4)
    def _():
        for d in range(1, 8):
            top(d).wait_send()
        for d in range(1, 16):

            @pl.when((g + d) % 16 != 0)
            def _():
                part(d).wait_send()

    @pl.when(g != 0)
    def _():
        for d in range(1, 8):
            panel(d).wait_send()

    for j in range(8):

        @pl.when(2 * j + core != 0)
        def _():
            panel_over(j).wait_send()

        @pl.when(2 * j + 1 - core != 0)
        def _():
            remote(m21.at[g], m21.at[2 * j + 1 - core], 11, 0, j, partner).wait_recv()

    upper = split(ui[...])
    for i in range(2):
        cols = [m21[8 * i : 8 * i + 8, j % 2, j // 2].reshape(512, 128) for j in range(4)]
        got = dot3(split(jnp.concatenate(cols, 1)), upper)
        lf[i] = got
        lh[i], ll[i] = split(got)

    own = pl.ds(pl.multiple_of(jnp.minimum(g, 3) * 128, 128), 128)

    def finish(d, _):
        p = (m + d) % 8
        i, q = p // 4, p % 4
        lanes = pl.ds(pl.multiple_of(128 * q, 128), 128)
        got = dot3((lh[i], ll[i]), (uh[:, lanes], ul[:, lanes]))
        z[p] = t[p] - got.reshape(2, 256, 128)

        @pl.when((q == 0) & (g < 4))
        def _():
            z[p] = lf[i, :, own].reshape(2, 256, 128)

        @pl.when(i == 0)
        def _():
            z[p, 0, 0:64] = uf[rows(m, 64), lanes]

        @pl.when((p == 0) & (g < 4))
        def _():
            z[p, 0, 0:64] = packed[rows(m, 64), own]

        @pl.when(d < 8)
        def _():
            back(d, True).start()
            back(d, False).start()

        return 0

    lax.fori_loop(1, 9, finish, 0)
    o[:, rows(m, 64)] = z[m, :, 0:64]
    o[:, rows(m, 192, 512)] = z[m, :, 64:256]
    for d in range(1, 8):
        back(d, True).wait()
        back(d, False).wait()


def spread(x):
    return jnp.concatenate([x[:512].reshape(8, 64), x[512:].reshape(8, 192)], 1)


def shards(matrix, row_diag, col_diag):
    scales = [spread(row_diag[l, 2048 * h : 2048 * h + 2048]) for l in range(2) for h in range(2)]
    scales = jnp.stack(scales, 1).reshape(8, 8, 128)
    across = jnp.broadcast_to(jnp.pad(col_diag, ((0, 6), (0, 0)))[None], (8, 8, 128))
    f32, bf16 = jnp.float32, jnp.bfloat16
    shapes = [
        ((8, 2, 256, 128), f32),
        ((8, 16, 128), f32),
        ((2, 2, 2, 256, 128), f32),
        ((8, 2, 256, 128), f32),
        ((8, 2, 2, 64, 128), f32),
        ((8, 4, 64, 128), f32),
        ((16, 2, 2, 64, 128), f32),
        ((512, 512), f32),
        ((512, 512), f32),
        ((512, 512), f32),
        ((2, 512, 512), bf16),
        ((2, 512, 512), bf16),
        ((2, 512, 512), f32),
        ((512, 512), f32),
        ((512, 512), bf16),
        ((512, 512), bf16),
        ((8, 2, 256, 128), f32),
    ]
    out = pl.pallas_call(
        kernel,
        out_shape=jax.ShapeDtypeStruct((2, 2048, 128), f32),
        in_specs=[VMEM] * 2,
        out_specs=VMEM,
        scratch_shapes=[pltpu.VMEM(*shape) for shape in shapes]
        + [pltpu.SemaphoreType.DMA((14, 16))] * 2,
        compiler_params=pltpu.CompilerParams(collective_id=0, has_side_effects=True),
        name="whole",
    )(matrix.reshape(2, 2048, 128), jnp.concatenate([scales, across], 1))
    return out.reshape(4096, 128)


def solution(mesh):
    in_specs = (P("row", "col"), P(None, "row"), P(None, "col"))
    out_specs = P("row", "col")
    return jax.shard_map(shards, mesh=mesh, in_specs=in_specs, out_specs=out_specs, check_vma=False)
```

```python
import functools

import jax
import jax.numpy as jnp
from jax import lax
from jax.experimental import pallas as pl
from jax.experimental.pallas import tpu as pltpu
from jax.sharding import PartitionSpec as P

MESH = pl.DeviceIdType.MESH
VMEM = pl.BlockSpec(memory_space=pltpu.VMEM)
GROUP = 4
EARLY = (1, 2, 4, 6)


def split(a):
    high = a.astype(jnp.bfloat16)
    return high, (a - high.astype(jnp.float32)).astype(jnp.bfloat16)


def dot(a, b):
    return jnp.dot(a, b, preferred_element_type=jnp.float32)


def dot3(a, b):
    return dot(a[0], b[0]) + (dot(a[0], b[1]) + dot(a[1], b[0]))


def rows_to(x, height):
    return jnp.broadcast_to(x, (height, x.shape[1]))


def lane_to(x, lane):
    return jnp.broadcast_to(x[:, lane : lane + 1], (x.shape[0], 128))


def lu128(s):
    height = 8 * GROUP
    sub = lax.broadcasted_iota(jnp.int32, (8, 128), 0)
    lane = lax.broadcasted_iota(jnp.int32, (8, 128), 1)
    subs = lax.broadcasted_iota(jnp.int32, (height, 128), 0)
    lanes = lax.broadcasted_iota(jnp.int32, (height, 128), 1)
    count = 16 // GROUP
    tiles = [s[height * t : height * t + height] for t in range(count)]
    extra = [jnp.where(lanes == subs + height * t, 1.0, 0.0) for t in range(count)]
    packed, lower = [], []

    def tall(x):
        return jnp.concatenate([x] * GROUP, 0)

    for b in range(16):
        at, part = b // GROUP, 8 * (b % GROUP)
        rows, rows2 = tiles[at][part : part + 8], extra[at][part : part + 8]
        cols = [lane_to(rows, 8 * b + c) for c in range(8)]
        inv, u = [], {}
        for c in range(8):
            r = 1.0 / rows_to(cols[c][c : c + 1], 8)
            inv.append(tall(r))
            factor = jnp.where(sub > c, cols[c] * r, 0.0)
            top = jnp.where(lane > 8 * b + c, rows_to(rows[c : c + 1], 8), 0.0)
            rows = jnp.where((lane == 8 * b + c) & (sub > c), factor, rows - factor * top)
            if c < 7:
                rows2 = rows2 - factor * rows_to(rows2[c : c + 1], 8)
            for d in range(c + 1, 8):
                row = rows_to(cols[d][c : c + 1], 8)
                u[c, d] = tall(row)
                cols[d] = cols[d] - factor * row
        packed.append(rows)
        lower.append(rows2)
        pieces = [jnp.where(lane == sub + 8 * b, 1.0, 0.0)]
        if part:
            pieces = [tiles[at][:part]] + pieces
        if part + 8 < height:
            pieces = pieces + [tiles[at][part + 8 :]]
        tiles[at] = jnp.concatenate(pieces, 0) if len(pieces) > 1 else pieces[0]
        inside = (lanes >= 8 * b) & (lanes < 8 * b + 8)
        ups, ups2 = [], []
        for c in range(8):
            top = jnp.where(lane >= 8 * b + 8, rows_to(rows[c : c + 1], 8), 0.0)
            ups.append(tall(jnp.where(lane == 8 * b + c, -1.0, top)))
            ups2.append(tall(rows_to(rows2[c : c + 1], 8)))
        for i in range(count):
            t = ((b + 1) // GROUP + i) % count
            tile = tiles[t]
            ls = [lane_to(tile, 8 * b + c) for c in range(8)]
            for c in range(8):
                ls[c] = ls[c] * inv[c]
                for d in range(c + 1, 8):
                    ls[d] = ls[d] - ls[c] * u[c, d]
            tile = jnp.where(inside, 0.0, tile)
            for c in range(8):
                tile = tile - ls[c] * ups[c]
            tiles[t] = tile
            if (t + 1) * GROUP - 1 > b:
                tile = extra[t]
                for c in range(8):
                    tile = tile - ls[c] * ups2[c]
                extra[t] = tile
    return tuple(jnp.concatenate(x, 0) for x in (packed, lower, tiles))


def lu_step(k, packed, li, ui):
    n = ui.shape[0]
    o = pl.multiple_of(k * 128, 128)
    blk = pl.ds(o, 128)
    own, lower, upper = lu128(ui[blk, blk])
    lower, upper = split(lower), split(upper)
    past = lax.broadcasted_iota(jnp.int32, (128, n), 1) >= o + 128
    diag = lax.broadcasted_iota(jnp.int32, (128, n), 1) == (
        lax.broadcasted_iota(jnp.int32, (128, n), 0) + o
    )
    band = ui[blk, :]
    right = dot3(lower, split(band))
    packed[blk, :] = jnp.where(past, right, band)
    packed[blk, blk] = own
    ui[blk, :] = jnp.where(diag, 1.0, 0.0)
    left = dot3(split(ui[:, blk]), upper)
    ui[...] = ui[...] - dot3(split(left), split(jnp.where(past, right, 0.0)))
    ui[:, blk] = left
    lband = dot3(lower, split(li[blk, :]))
    li[blk, :] = lband
    below = lax.broadcasted_iota(jnp.int32, (n, 128), 0) >= o + 128
    li[...] = li[...] - dot3(split(jnp.where(below, left, 0.0)), split(lband))


def kernel(hbm, rd, cd, o, x, rdo, cds, xin, rs, t, m11, m12, m21, packed, li, ui, lh, ll, lf, uf, uh, ul, z, send, recv, load):
    r, c = lax.axis_index("row"), lax.axis_index("col")
    q, g = c // 16, c % 16
    m = r * 4 + q
    core, pair = g % 2, g // 2

    def member(p):
        return {"row": p // 4, "col": (p % 4) * 16 + g}

    def chip(d):
        return {"row": r, "col": (m % 4) * 16 + (g + 2 * d) % 16}

    partner = {"row": r, "col": (m % 4) * 16 + g + 1 - 2 * core}

    def device(p):
        return {"row": r, "col": (m % 4) * 16 + p}

    def remote(src, dst, kind, out, into, where):
        return pltpu.make_async_remote_copy(
            src, dst, send.at[kind, out], recv.at[kind, into], device_id=where, device_id_type=MESH
        )

    def rows(p, height, base=0):
        return pl.ds(pl.multiple_of(base + height * p, 8), height)

    def head(d):
        p = (m + d) % 8
        return remote(x.at[:, rows(p, 64)], xin.at[m, :, pl.ds(0, 64)], 0, d, d, member(p))

    def small(d):
        if d == 0:
            return remote(rd, rdo, 1, 0, 0, member((m + 4) % 8))
        return remote(cd, cds.at[q], 1, d, d, member(r * 4 + (q + d) % 4))

    def tail(d, half):
        p = (m + d) % 8
        return remote(
            x.at[half, rows(p, 192, 512)], xin.at[m, half, pl.ds(64, 192)], 2 + half, d, d, member(p)
        )

    def top(d):
        return remote(t.at[0, 0, pl.ds(0, 64)], m21.at[0, core, pair], 4, d, pair, chip(d))

    def top_over():
        return remote(m21.at[0, core], m21.at[0, core], 5, 0, 0, partner)

    def corner(d):
        return remote(m21.at[0, core], m11.at[m, core], 6, d, d, member((m + d) % 8))

    def corner_over(d):
        p = (m + 8 - d) % 8
        return remote(m11.at[p, core], m11.at[p, core], 7, d, d, partner)

    def band(d):
        return remote(t.at[pl.ds(0, 4), 0, pl.ds(0, 64)], m12.at[m], 8, d, d, member((m + d) % 8))

    def piece(p):
        return t.at[(p // 8) * 4, (p % 8) // 4, rows(p % 4, 64)]

    def part(d):
        p = (g + d) % 16
        return remote(piece(p), m21.at[p, core, pair], 9, d, g, device(p))

    def panel(d):
        return remote(m21.at[g], m21.at[g], 10, d, pair, chip(d))

    def panel_over(j):
        p = 2 * j + core
        return remote(m21.at[p], m21.at[p], 11, j, j, partner)

    def target(slot):
        half = slot // 4
        return 4 * ((r + 1 + half) % 2) + (q + slot + half) % 4

    def back(slot, first):
        p = target(slot)
        if first:
            return remote(z.at[p, :, pl.ds(0, 64)], o.at[:, rows(m, 64)], 12, slot, slot, member(p))
        return remote(z.at[p, :, pl.ds(64, 192)], o.at[:, rows(m, 192, 512)], 13, slot, slot, member(p))

    loads = [
        pltpu.make_async_copy(hbm.at[:, pl.ds(0, 512)], x.at[:, pl.ds(0, 512)], load.at[0]),
        pltpu.make_async_copy(hbm.at[:, pl.ds(512, 1536)], x.at[:, pl.ds(512, 1536)], load.at[1]),
    ]
    for copy in loads:
        copy.start()

    bar = pltpu.get_barrier_semaphore()
    for d in range(1, 8):
        pl.semaphore_signal(bar, inc=1, device_id=member((m + d) % 8), device_id_type=MESH)
    for d in range(1, 16):
        pl.semaphore_signal(bar, inc=1, device_id=device((g + d) % 16), device_id_type=MESH)
    pl.semaphore_wait(bar, 22)

    for d in range(4):
        small(d).start()
    loads[0].wait()
    for d in range(1, 8):
        head(d).start()
    cds[q] = cd[...]
    xin[m, :, 0:64] = x[:, rows(m, 64)]
    loads[1].wait()
    for d in EARLY:
        tail(d, 0).start()
    xin[m, :, 64:256] = x[:, rows(m, 192, 512)]

    def widen(source, i):
        for l in range(2):
            for h in range(2):
                for j in range(3):
                    at = 16 * h + (m // 2 if j == 0 else 3 + j + 3 * m // 2)
                    line = source[l : l + 1, pl.ds(pl.multiple_of(128 * at, 128), 128)]
                    rs[l, i, h, 128 * j : 128 * j + 128] = rows_to(line, 128).T

    widen(rd, r)
    for d in range(4):
        small(d).wait()
    widen(rdo, 1 - r)

    def mix(base, j, _):
        at = pl.ds(pl.multiple_of(8 * j, 8), 8)
        to = pl.ds(pl.multiple_of(8 * j + base + 64 * (m % 2), 8), 8)
        first = [rows_to(cds[q, 0:1, :], 8) for q in range(4)]
        second = [rows_to(cds[q, 1:2, :] * 0.25, 8) for q in range(4)]
        for i in range(2):
            mid = {}
            for q in range(4):
                y = []
                for h in range(2):
                    a, b = xin[q, h, at], xin[4 + q, h, at]
                    y.append(rs[0, i, h, to] * (a + b if i == 0 else a - b))
                mid[q] = [rs[1, i, 0, to] * (y[0] + y[1]), rs[1, i, 1, to] * (y[0] - y[1])]
            for h in range(2):
                w = [first[q] * (mid[q][h] + mid[q + 2][h]) for q in range(2)]
                w += [first[q + 2] * (mid[q][h] - mid[q + 2][h]) for q in range(2)]
                for q in (0, 2):
                    t[4 * i + q, h, at] = second[q] * (w[q] + w[q + 1])
                    t[4 * i + q + 1, h, at] = second[q + 1] * (w[q] - w[q + 1])
        return 0

    for d in range(1, 8):
        head(d).wait()
    lax.fori_loop(0, 8, functools.partial(mix, 0), 0)

    @pl.when(g < 4)
    def _():
        for d in range(1, 8):
            top(d).start()
        m21[0, core, pair] = t[0, 0, 0:64]

    for i in range(2):

        @pl.when(g != 2 * i + core)
        def _():
            remote(t.at[0, 0, pl.ds(0, 64)], m21.at[0, core, i], 4, 0, i, partner).wait_recv()

    for d in range(1, 8):
        corner(d).start()
    top_over().start()
    for d in range(1, 8):
        if d not in EARLY:
            tail(d, 0).start()
        tail(d, 1).start()
    for d in range(1, 8):
        band(d).start()
    m11[m, core] = m21[0, core]
    m12[m] = t[0:4, 0, 0:64]
    li[...] = jnp.where(
        lax.broadcasted_iota(jnp.int32, li.shape, 0) == lax.broadcasted_iota(jnp.int32, li.shape, 1),
        1.0,
        0.0,
    )
    top_over().wait()
    m11[m, 1 - core] = m21[0, 1 - core]
    for d in range(1, 8):
        corner(d).wait_recv()
        corner_over(d).start()
    for d in range(1, 8):
        corner_over(d).wait()
    for i in range(8):
        for j in range(4):
            ui[64 * i : 64 * i + 64, 128 * j : 128 * j + 128] = m11[i, j % 2, j // 2]

    def eliminate(k, _):
        lu_step(k, packed, li, ui)

        @pl.when(k == 0)
        def _():
            for d in range(1, 8):
                tail(d, 0).wait()
                tail(d, 1).wait()
            lax.fori_loop(8, 32, functools.partial(mix, 64), 0)

            @pl.when(g < 4)
            def _():
                for d in range(1, 16):

                    @pl.when((g + d) % 16 != 0)
                    def _():
                        part(d).start()

                @pl.when(g != 0)
                def _():
                    m21[g, core, pair] = t[0, 0, rows(g, 64)]

        @pl.when(k == 1)
        def _():
            @pl.when(g != 0)
            def _():
                for i in range(4):

                    @pl.when(g != i)
                    def _():
                        remote(
                            piece(g), m21.at[g, i % 2, i // 2], 9, 0, i, partner
                        ).wait_recv()

                for d in range(1, 8):
                    panel(d).start()
                panel_over(pair).start()

        return 0

    lax.fori_loop(0, 4, eliminate, 0)

    def relay(i):
        for k in range(4):
            j = 4 * i + k

            @pl.when((2 * j + core != 0) & (j != pair))
            def _():
                remote(m21.at[g], m21.at[2 * j + core], 10, 0, j, partner).wait_recv()
                panel_over(j).start()

    def left_of(i):
        for k in range(4):
            j = 4 * i + k

            @pl.when(2 * j + 1 - core != 0)
            def _():
                remote(m21.at[g], m21.at[2 * j + 1 - core], 11, 0, j, partner).wait_recv()

        at = pl.ds(8 * i, 8)
        cols = [m21[at, j % 2, j // 2].reshape(512, 128) for j in range(4)]
        got = dot3(split(jnp.concatenate(cols, 1)), split(ui[...]))
        lf[i] = got
        lh[i], ll[i] = split(got)

    own = pl.ds(pl.multiple_of(jnp.minimum(g, 3) * 128, 128), 128)

    def finish(slot, _):
        p = target(slot)
        i = p // 4
        lanes = pl.ds(pl.multiple_of(128 * (p % 4), 128), 128)
        got = dot3((lh[i], ll[i]), (uh[:, lanes], ul[:, lanes]))
        z[p] = t[p] - got.reshape(2, 256, 128)

        @pl.when((p % 4 == 0) & (g < 4))
        def _():
            z[p] = lf[i, :, own].reshape(2, 256, 128)

        @pl.when(i == 0)
        def _():
            z[p, 0, 0:64] = uf[rows(m, 64), lanes]

        @pl.when((p == 0) & (g < 4))
        def _():
            z[p, 0, 0:64] = packed[rows(m, 64), own]

        @pl.when(slot < 7)
        def _():
            back(slot, True).start()
            back(slot, False).start()

        return 0

    relay(1 - r)
    for d in range(1, 8):
        band(d).wait()
    lower = split(li[...])
    for j in range(4):
        lanes = slice(128 * j, 128 * j + 128)
        uf[:, lanes] = dot3(lower, split(m12[:, j].reshape(512, 128)))
        uh[:, lanes], ul[:, lanes] = split(uf[:, lanes])
    left_of(1 - r)
    relay(r)
    lax.fori_loop(0, 4, finish, 0)
    left_of(r)
    lax.fori_loop(4, 8, finish, 0)
    o[:, rows(m, 64)] = z[m, :, 0:64]
    o[:, rows(m, 192, 512)] = z[m, :, 64:256]

    for d in range(1, 8):
        corner(d).wait_send()

    @pl.when(g < 4)
    def _():
        for d in range(1, 8):
            top(d).wait_send()
        for d in range(1, 16):

            @pl.when((g + d) % 16 != 0)
            def _():
                part(d).wait_send()

    @pl.when(g != 0)
    def _():
        for d in range(1, 8):
            panel(d).wait_send()

    for j in range(8):

        @pl.when(2 * j + core != 0)
        def _():
            panel_over(j).wait_send()

    for slot in range(7):
        back(slot, True).wait()
        back(slot, False).wait()


def shards(matrix, row_diag, col_diag):
    f32, bf16 = jnp.float32, jnp.bfloat16
    shapes = [
        ((2, 2048, 128), f32),
        ((2, 4096), f32),
        ((4, 2, 128), f32),
        ((8, 2, 256, 128), f32),
        ((2, 2, 2, 384, 128), f32),
        ((8, 2, 256, 128), f32),
        ((8, 2, 2, 64, 128), f32),
        ((8, 4, 64, 128), f32),
        ((16, 2, 2, 64, 128), f32),
        ((512, 512), f32),
        ((512, 512), f32),
        ((512, 512), f32),
        ((2, 512, 512), bf16),
        ((2, 512, 512), bf16),
        ((2, 512, 512), f32),
        ((512, 512), f32),
        ((512, 512), bf16),
        ((512, 512), bf16),
        ((8, 2, 256, 128), f32),
    ]
    out = pl.pallas_call(
        kernel,
        out_shape=pltpu.VMEM((2, 2048, 128), f32),
        in_specs=[pl.BlockSpec(memory_space=pl.ANY), VMEM, VMEM],
        out_specs=VMEM,
        scratch_shapes=[pltpu.VMEM(*shape) for shape in shapes]
        + [pltpu.SemaphoreType.DMA((14, 16))] * 2
        + [pltpu.SemaphoreType.DMA((2,))],
        compiler_params=pltpu.CompilerParams(collective_id=0, has_side_effects=True),
        name="whole",
    )(matrix.reshape(2, 2048, 128), row_diag, col_diag)
    return out.reshape(4096, 128)


def solution(mesh):
    in_specs = (P("row", "col"), P(None, "row"), P(None, "col"))
    out_specs = P("row", "col")
    return jax.shard_map(shards, mesh=mesh, in_specs=in_specs, out_specs=out_specs, check_vma=False)
```

```python
import functools

import jax
import jax.numpy as jnp
from jax import lax
from jax.experimental import pallas as pl
from jax.experimental.pallas import tpu as pltpu
from jax.sharding import PartitionSpec as P

MESH = pl.DeviceIdType.MESH
VMEM = pl.BlockSpec(memory_space=pltpu.VMEM)
GROUP = 4
EARLY = (1, 2, 4, 6)


def split(a):
    high = a.astype(jnp.bfloat16)
    return high, (a - high.astype(jnp.float32)).astype(jnp.bfloat16)


def dot(a, b):
    return jnp.dot(a, b, preferred_element_type=jnp.float32)


def dot3(a, b):
    return dot(a[0], b[0]) + (dot(a[0], b[1]) + dot(a[1], b[0]))


def rows_to(x, height):
    return jnp.broadcast_to(x, (height, x.shape[1]))


def lane_to(x, lane):
    return jnp.broadcast_to(x[:, lane : lane + 1], (x.shape[0], 128))


def lu128(s):
    height = 8 * GROUP
    sub = lax.broadcasted_iota(jnp.int32, (8, 128), 0)
    lane = lax.broadcasted_iota(jnp.int32, (8, 128), 1)
    subs = lax.broadcasted_iota(jnp.int32, (height, 128), 0)
    lanes = lax.broadcasted_iota(jnp.int32, (height, 128), 1)
    count = 16 // GROUP
    tiles = [s[height * t : height * t + height] for t in range(count)]
    extra = [jnp.where(lanes == subs + height * t, 1.0, 0.0) for t in range(count)]
    packed, lower = [], []

    def tall(x):
        return jnp.concatenate([x] * GROUP, 0)

    for b in range(16):
        at, part = b // GROUP, 8 * (b % GROUP)
        rows, rows2 = tiles[at][part : part + 8], extra[at][part : part + 8]
        cols = [lane_to(rows, 8 * b + c) for c in range(8)]
        inner = (lane >= 8 * b) & (lane < 8 * b + 8)
        full = jnp.where(lane >= 8 * b + 8, rows, jnp.where(lane == sub + 8 * b, -1.0, 0.0))
        full2 = rows2
        for c in range(8):
            column = cols[c]
            r = 1.0 / rows_to(column[c : c + 1], 8)
            factor = jnp.where(sub > c, column * r, 0.0)
            for d in range(c + 1, 8):
                row = rows_to(cols[d][c : c + 1], 8) * r
                cols[d] = jnp.where(sub == c, row, cols[d] - column * row)
            row = rows_to(full[c : c + 1], 8) * r
            full = jnp.where(sub == c, row, full - jnp.where(inner & (sub > c), 0.0, column) * row)
            row = rows_to(full2[c : c + 1], 8) * r
            full2 = jnp.where(sub == c, row, full2 - column * row)
            top = jnp.where(lane > 8 * b + c, rows_to(rows[c : c + 1], 8), 0.0)
            rows = jnp.where((lane == 8 * b + c) & (sub > c), factor, rows - factor * top)
            if c < 7:
                rows2 = rows2 - factor * rows_to(rows2[c : c + 1], 8)
        packed.append(rows)
        lower.append(rows2)
        pieces = [jnp.where(lane == sub + 8 * b, 1.0, 0.0)]
        if part:
            pieces = [tiles[at][:part]] + pieces
        if part + 8 < height:
            pieces = pieces + [tiles[at][part + 8 :]]
        tiles[at] = jnp.concatenate(pieces, 0) if len(pieces) > 1 else pieces[0]
        inside = (lanes >= 8 * b) & (lanes < 8 * b + 8)
        ups = [tall(rows_to(full[c : c + 1], 8)) for c in range(8)]
        ups2 = [tall(rows_to(full2[c : c + 1], 8)) for c in range(8)]
        for i in range(count):
            t = ((b + 1) // GROUP + i) % count
            tile = tiles[t]
            ls = [lane_to(tile, 8 * b + c) for c in range(8)]
            tile = jnp.where(inside, 0.0, tile)
            for c in range(8):
                tile = tile - ls[c] * ups[c]
            tiles[t] = tile
            if (t + 1) * GROUP - 1 > b:
                tile = extra[t]
                for c in range(8):
                    tile = tile - ls[c] * ups2[c]
                extra[t] = tile
    return tuple(jnp.concatenate(x, 0) for x in (packed, lower, tiles))


def lu_step(k, packed, li, ui):
    n = ui.shape[0]
    o = pl.multiple_of(k * 128, 128)
    blk = pl.ds(o, 128)
    own, lower, upper = lu128(ui[blk, blk])
    lower, upper = split(lower), split(upper)
    past = lax.broadcasted_iota(jnp.int32, (128, n), 1) >= o + 128
    diag = lax.broadcasted_iota(jnp.int32, (128, n), 1) == (
        lax.broadcasted_iota(jnp.int32, (128, n), 0) + o
    )
    band = ui[blk, :]
    right = dot3(lower, split(band))
    packed[blk, :] = jnp.where(past, right, band)
    packed[blk, blk] = own
    ui[blk, :] = jnp.where(diag, 1.0, 0.0)
    left = dot3(split(ui[:, blk]), upper)
    ui[...] = ui[...] - dot3(split(left), split(jnp.where(past, right, 0.0)))
    ui[:, blk] = left
    lband = dot3(lower, split(li[blk, :]))
    li[blk, :] = lband
    below = lax.broadcasted_iota(jnp.int32, (n, 128), 0) >= o + 128
    li[...] = li[...] - dot3(split(jnp.where(below, left, 0.0)), split(lband))


def kernel(hbm, rd, cd, o, x, rdo, cds, xin, rs, t, m11, m12, m21, packed, li, ui, mh, ml, uf, wh, wl, lih, lil, uih, uil, z, send, recv, load):
    r, c = lax.axis_index("row"), lax.axis_index("col")
    q, g = c // 16, c % 16
    m = r * 4 + q
    core, pair = g % 2, g // 2

    def member(p):
        return {"row": p // 4, "col": (p % 4) * 16 + g}

    def chip(d):
        return {"row": r, "col": (m % 4) * 16 + (g + 2 * d) % 16}

    partner = {"row": r, "col": (m % 4) * 16 + g + 1 - 2 * core}

    def device(p):
        return {"row": r, "col": (m % 4) * 16 + p}

    def remote(src, dst, kind, out, into, where):
        return pltpu.make_async_remote_copy(
            src, dst, send.at[kind, out], recv.at[kind, into], device_id=where, device_id_type=MESH
        )

    def rows(p, height, base=0):
        return pl.ds(pl.multiple_of(base + height * p, 8), height)

    def head(d):
        p = (m + d) % 8
        return remote(x.at[:, rows(p, 64)], xin.at[m, :, pl.ds(0, 64)], 0, d, d, member(p))

    def small(d):
        if d == 0:
            return remote(rd, rdo, 1, 0, 0, member((m + 4) % 8))
        return remote(cd, cds.at[q], 1, d, d, member(r * 4 + (q + d) % 4))

    def tail(d, unit):
        p = (m + d) % 8
        return remote(
            x.at[:, pl.ds(pl.multiple_of(192 * p + 448 + 64 * unit, 8), 64)],
            xin.at[m, :, pl.ds(64 * unit, 64)],
            (0, 2, 3, 14)[unit],
            d,
            d,
            member(p),
        )

    def top(d):
        return remote(t.at[0, 0, pl.ds(0, 64)], m21.at[0, core, pair], 4, d, pair, chip(d))

    def top_over():
        return remote(m21.at[0, core], m21.at[0, core], 5, 0, 0, partner)

    def corner(d):
        return remote(m21.at[0, core], m11.at[m, core], 6, d, d, member((m + d) % 8))

    def corner_over(d):
        p = (m + 8 - d) % 8
        return remote(m11.at[p, core], m11.at[p, core], 7, d, d, partner)

    def band(d):
        return remote(t.at[pl.ds(0, 4), 0, pl.ds(0, 64)], m12.at[m], 8, d, d, member((m + d) % 8))

    def piece(p):
        return t.at[(p // 8) * 4, (p % 8) // 4, rows(p % 4, 64)]

    def part(p, plane):
        return pltpu.make_async_remote_copy(
            piece(p),
            m21.at[p, core, pair],
            send.at[9 + 6 * plane, p],
            recv.at[9, g + 4 * (p // 8)],
            device_id=device(8 * plane + p % 8),
            device_id_type=MESH,
        )

    def parts(unit):
        @pl.when(g < 4)
        def _():
            for i in range(4):
                p = 4 * i + unit
                if p == 0:
                    continue
                part(p, 1).start()
                if p % 8 >= 4:
                    part(p, 0).start()
                else:

                    @pl.when(g != p % 8)
                    def _():
                        part(p, 0).start()

                    @pl.when(g == p % 8)
                    def _():
                        m21[p, core, pair] = piece(p)[...]

    def spread(unit):
        @pl.when(g % 4 == unit)
        def _():
            for e in range(2):

                @pl.when(here + 8 * e != 0)
                def _():
                    for i in range(4):

                        @pl.when(g != i)
                        def _():
                            remote(
                                piece(here), m21.at[here + 8 * e, i % 2, i // 2], 9, 0, i + 4 * e, partner
                            ).wait_recv()

                    for d in range(1, 4):
                        panel(e, d).start()
                    panel_over(here // 2 + 4 * e).start()

    def arrive(unit):
        for d in range(1, 8):
            tail(d, unit).wait()
        lax.fori_loop(8 * unit, 8 * unit + 8, functools.partial(mix, 64), 0)

    here = g % 8

    def panel(e, d):
        p = here + 8 * e
        where = device(8 * (g // 8) + (here + 2 * d) % 8)
        return remote(m21.at[p], m21.at[p], 10, 4 * e + d, here // 2 + 4 * e, where)

    def panel_over(j):
        p = 2 * j + core
        return remote(m21.at[p], m21.at[p], 11, j, j, partner)

    def target(slot):
        half = slot // 4
        return 4 * ((r + 1 + half) % 2) + (q + slot + half) % 4

    def back(slot, first):
        p = target(slot)
        if first:
            return remote(z.at[p, :, pl.ds(0, 64)], o.at[:, rows(m, 64)], 12, slot, slot, member(p))
        return remote(z.at[p, :, pl.ds(64, 192)], o.at[:, rows(m, 192, 512)], 13, slot, slot, member(p))

    loads = [
        pltpu.make_async_copy(hbm.at[:, pl.ds(0, 512)], x.at[:, pl.ds(0, 512)], load.at[0]),
        pltpu.make_async_copy(hbm.at[:, pl.ds(512, 1536)], x.at[:, pl.ds(512, 1536)], load.at[1]),
    ]
    for copy in loads:
        copy.start()

    bar = pltpu.get_barrier_semaphore()
    for d in range(1, 8):
        pl.semaphore_signal(bar, inc=1, device_id=member((m + d) % 8), device_id_type=MESH)
    for d in range(1, 16):
        pl.semaphore_signal(bar, inc=1, device_id=device((g + d) % 16), device_id_type=MESH)
    pl.semaphore_wait(bar, 22)

    for d in range(4):
        small(d).start()
    loads[0].wait()
    for d in range(1, 8):
        head(d).start()
    cds[q] = cd[...]
    xin[m, :, 0:64] = x[:, rows(m, 64)]
    loads[1].wait()
    for d in EARLY:
        tail(d, 1).start()
    xin[m, :, 64:256] = x[:, rows(m, 192, 512)]

    def widen(source, i):
        for l in range(2):
            for h in range(2):
                for j in range(3):
                    at = 16 * h + (m // 2 if j == 0 else 3 + j + 3 * m // 2)
                    line = source[l : l + 1, pl.ds(pl.multiple_of(128 * at, 128), 128)]
                    rs[l, i, h, 128 * j : 128 * j + 128] = rows_to(line, 128).T

    widen(rd, r)
    for d in range(4):
        small(d).wait()
    widen(rdo, 1 - r)

    def mix(base, j, _):
        at = pl.ds(pl.multiple_of(8 * j, 8), 8)
        to = pl.ds(pl.multiple_of(8 * j + base + 64 * (m % 2), 8), 8)
        first = [rows_to(cds[q, 0:1, :], 8) for q in range(4)]
        second = [rows_to(cds[q, 1:2, :] * 0.25, 8) for q in range(4)]
        for i in range(2):
            mid = {}
            for q in range(4):
                y = []
                for h in range(2):
                    a, b = xin[q, h, at], xin[4 + q, h, at]
                    y.append(rs[0, i, h, to] * (a + b if i == 0 else a - b))
                mid[q] = [rs[1, i, 0, to] * (y[0] + y[1]), rs[1, i, 1, to] * (y[0] - y[1])]
            for h in range(2):
                w = [first[q] * (mid[q][h] + mid[q + 2][h]) for q in range(2)]
                w += [first[q + 2] * (mid[q][h] - mid[q + 2][h]) for q in range(2)]
                for q in (0, 2):
                    t[4 * i + q, h, at] = second[q] * (w[q] + w[q + 1])
                    t[4 * i + q + 1, h, at] = second[q + 1] * (w[q] - w[q + 1])
        return 0

    for d in range(1, 8):
        head(d).wait()
    lax.fori_loop(0, 8, functools.partial(mix, 0), 0)

    @pl.when(g < 4)
    def _():
        for d in range(1, 8):
            top(d).start()
        m21[0, core, pair] = t[0, 0, 0:64]

    parts(0)

    for i in range(2):

        @pl.when(g != 2 * i + core)
        def _():
            remote(t.at[0, 0, pl.ds(0, 64)], m21.at[0, core, i], 4, 0, i, partner).wait_recv()

    for d in range(1, 8):
        corner(d).start()
    top_over().start()
    for d in range(1, 8):
        if d not in EARLY:
            tail(d, 1).start()
    for unit in (2, 3):
        for d in range(1, 8):
            tail(d, unit).start()
    m11[m, core] = m21[0, core]
    m12[m] = t[0:4, 0, 0:64]
    li[...] = jnp.where(
        lax.broadcasted_iota(jnp.int32, li.shape, 0) == lax.broadcasted_iota(jnp.int32, li.shape, 1),
        1.0,
        0.0,
    )
    top_over().wait()
    m11[m, 1 - core] = m21[0, 1 - core]
    for d in range(1, 8):
        corner(d).wait_recv()
        corner_over(d).start()
    for d in range(1, 8):
        corner_over(d).wait()
    for i in range(8):
        for j in range(4):
            ui[64 * i : 64 * i + 64, 128 * j : 128 * j + 128] = m11[i, j % 2, j // 2]

    spread(0)

    def eliminate(k, _):
        lu_step(k, packed, li, ui)

        @pl.when(k == 0)
        def _():
            arrive(1)
            parts(1)
            arrive(2)
            parts(2)
            for d in range(1, 8):
                band(d).start()

        @pl.when(k == 1)
        def _():
            arrive(3)
            parts(3)
            spread(1)
            spread(2)

        @pl.when(k == 2)
        def _():
            spread(3)

        return 0

    lax.fori_loop(0, 4, eliminate, 0)

    def relay(i):
        for k in range(4):
            j = 4 * i + k

            @pl.when((2 * j + core != 0) & (j != here // 2 + 4 * i))
            def _():
                remote(m21.at[here], m21.at[2 * j + core], 10, 0, j, partner).wait_recv()
                panel_over(j).start()

    def left_of(i):
        for k in range(4):
            j = 4 * i + k

            @pl.when(2 * j + 1 - core != 0)
            def _():
                remote(m21.at[here], m21.at[2 * j + 1 - core], 11, 0, j, partner).wait_recv()

        at = pl.ds(8 * i, 8)
        for j in range(4):
            lanes = slice(128 * j, 128 * j + 128)
            mh[i, :, lanes], ml[i, :, lanes] = split(m21[at, j % 2, j // 2].reshape(512, 128))

    own = pl.ds(pl.multiple_of(jnp.minimum(g, 3) * 128, 128), 128)

    def prepare(slot):
        j = (q + slot) % 4
        lanes = pl.ds(pl.multiple_of(128 * j, 128), 128)
        right = dot3((lih[...], lil[...]), split(m12[:, j].reshape(512, 128)))
        uf[:, lanes] = right
        wh[:, lanes], wl[:, lanes] = split(dot3((uih[...], uil[...]), split(right)))

    def finish(slot, _):
        p = target(slot)
        i = p // 4
        lanes = pl.ds(pl.multiple_of(128 * (p % 4), 128), 128)
        got = dot3((mh[i], ml[i]), (wh[:, lanes], wl[:, lanes]))
        z[p] = t[p] - got.reshape(2, 256, 128)

        @pl.when((p % 4 == 0) & (g < 4))
        def _():
            z[p] = dot3((mh[i], ml[i]), (uih[:, own], uil[:, own])).reshape(2, 256, 128)

        @pl.when(i == 0)
        def _():
            z[p, 0, 0:64] = uf[rows(m, 64), lanes]

        @pl.when((p == 0) & (g < 4))
        def _():
            z[p, 0, 0:64] = packed[rows(m, 64), own]

        @pl.when(slot < 7)
        def _():
            back(slot, True).start()
            back(slot, False).start()

        @pl.when(slot < 3)
        def _():
            prepare(slot + 1)

        return 0

    relay(1 - r)
    for d in range(1, 8):
        band(d).wait()
    lih[...], lil[...] = split(li[...])
    uih[...], uil[...] = split(ui[...])
    prepare(0)
    left_of(1 - r)
    relay(r)
    lax.fori_loop(0, 4, finish, 0)
    left_of(r)
    lax.fori_loop(4, 8, finish, 0)
    o[:, rows(m, 64)] = z[m, :, 0:64]
    o[:, rows(m, 192, 512)] = z[m, :, 64:256]

    for d in range(1, 8):
        corner(d).wait_send()

    @pl.when(g < 4)
    def _():
        for d in range(1, 8):
            top(d).wait_send()
        for p in range(1, 16):
            part(p, 1).wait_send()

            @pl.when(g != p % 8)
            def _():
                part(p, 0).wait_send()

    for e in range(2):

        @pl.when(here + 8 * e != 0)
        def _():
            for d in range(1, 4):
                panel(e, d).wait_send()

    for j in range(8):

        @pl.when(2 * j + core != 0)
        def _():
            panel_over(j).wait_send()

    for slot in range(7):
        back(slot, True).wait()
        back(slot, False).wait()


def shards(matrix, row_diag, col_diag):
    f32, bf16 = jnp.float32, jnp.bfloat16
    shapes = [
        ((2, 2048, 128), f32),
        ((2, 4096), f32),
        ((4, 2, 128), f32),
        ((8, 2, 256, 128), f32),
        ((2, 2, 2, 384, 128), f32),
        ((8, 2, 256, 128), f32),
        ((8, 2, 2, 64, 128), f32),
        ((8, 4, 64, 128), f32),
        ((16, 2, 2, 64, 128), f32),
        ((512, 512), f32),
        ((512, 512), f32),
        ((512, 512), f32),
        ((2, 512, 512), bf16),
        ((2, 512, 512), bf16),
        ((512, 512), f32),
        ((512, 512), bf16),
        ((512, 512), bf16),
        ((512, 512), bf16),
        ((512, 512), bf16),
        ((512, 512), bf16),
        ((512, 512), bf16),
        ((8, 2, 256, 128), f32),
    ]
    out = pl.pallas_call(
        kernel,
        out_shape=pltpu.VMEM((2, 2048, 128), f32),
        in_specs=[pl.BlockSpec(memory_space=pl.ANY), VMEM, VMEM],
        out_specs=VMEM,
        scratch_shapes=[pltpu.VMEM(*shape) for shape in shapes]
        + [pltpu.SemaphoreType.DMA((16, 16))] * 2
        + [pltpu.SemaphoreType.DMA((2,))],
        compiler_params=pltpu.CompilerParams(collective_id=0, has_side_effects=True),
        name="whole",
    )(matrix.reshape(2, 2048, 128), row_diag, col_diag)
    return out.reshape(4096, 128)


def solution(mesh):
    in_specs = (P("row", "col"), P(None, "row"), P(None, "col"))
    out_specs = P("row", "col")
    return jax.shard_map(shards, mesh=mesh, in_specs=in_specs, out_specs=out_specs, check_vma=False)
```

```python
import functools

import jax
import jax.numpy as jnp
from jax import lax
from jax.experimental import pallas as pl
from jax.experimental.pallas import tpu as pltpu
from jax.sharding import PartitionSpec as P

MESH = pl.DeviceIdType.MESH
VMEM = pl.BlockSpec(memory_space=pltpu.VMEM)
GROUP = 4
EARLY = (1, 2, 3, 4, 5, 6, 7)


def split(a):
    high = a.astype(jnp.bfloat16)
    return high, (a - high.astype(jnp.float32)).astype(jnp.bfloat16)


def dot(a, b):
    return jnp.dot(a, b, preferred_element_type=jnp.float32)


def dot3(a, b):
    return dot(a[0], b[0]) + (dot(a[0], b[1]) + dot(a[1], b[0]))


def rows_to(x, height):
    return jnp.broadcast_to(x, (height, x.shape[1]))


def lane_to(x, lane):
    return jnp.broadcast_to(x[:, lane : lane + 1], (x.shape[0], 128))


def lu128(s):
    height = 8 * GROUP
    sub = lax.broadcasted_iota(jnp.int32, (8, 128), 0)
    lane = lax.broadcasted_iota(jnp.int32, (8, 128), 1)
    subs = lax.broadcasted_iota(jnp.int32, (height, 128), 0)
    lanes = lax.broadcasted_iota(jnp.int32, (height, 128), 1)
    count = 16 // GROUP
    tiles = [s[height * t : height * t + height] for t in range(count)]
    extra = [jnp.where(lanes == subs + height * t, 1.0, 0.0) for t in range(count)]
    packed, lower = [], []

    def tall(x):
        return jnp.concatenate([x] * GROUP, 0)

    for b in range(16):
        at, part = b // GROUP, 8 * (b % GROUP)
        rows, rows2 = tiles[at][part : part + 8], extra[at][part : part + 8]
        cols = [lane_to(rows, 8 * b + c) for c in range(8)]
        inner = (lane >= 8 * b) & (lane < 8 * b + 8)
        full = jnp.where(lane >= 8 * b + 8, rows, jnp.where(lane == sub + 8 * b, -1.0, 0.0))
        full2 = rows2
        for c in range(8):
            column = cols[c]
            r = 1.0 / rows_to(column[c : c + 1], 8)
            factor = jnp.where(sub > c, column * r, 0.0)
            for d in range(c + 1, 8):
                row = rows_to(cols[d][c : c + 1], 8) * r
                cols[d] = jnp.where(sub == c, row, cols[d] - column * row)
            row = rows_to(full[c : c + 1], 8) * r
            full = jnp.where(sub == c, row, full - jnp.where(inner & (sub > c), 0.0, column) * row)
            row = rows_to(full2[c : c + 1], 8) * r
            full2 = jnp.where(sub == c, row, full2 - column * row)
            top = jnp.where(lane > 8 * b + c, rows_to(rows[c : c + 1], 8), 0.0)
            rows = jnp.where((lane == 8 * b + c) & (sub > c), factor, rows - factor * top)
            if c < 7:
                rows2 = rows2 - factor * rows_to(rows2[c : c + 1], 8)
        packed.append(rows)
        lower.append(rows2)
        pieces = [jnp.where(lane == sub + 8 * b, 1.0, 0.0)]
        if part:
            pieces = [tiles[at][:part]] + pieces
        if part + 8 < height:
            pieces = pieces + [tiles[at][part + 8 :]]
        tiles[at] = jnp.concatenate(pieces, 0) if len(pieces) > 1 else pieces[0]
        inside = (lanes >= 8 * b) & (lanes < 8 * b + 8)
        ups = [tall(rows_to(full[c : c + 1], 8)) for c in range(8)]
        ups2 = [tall(rows_to(full2[c : c + 1], 8)) for c in range(8)]
        for i in range(count):
            t = ((b + 1) // GROUP + i) % count
            tile = tiles[t]
            ls = [lane_to(tile, 8 * b + c) for c in range(8)]
            tile = jnp.where(inside, 0.0, tile)
            for c in range(8):
                tile = tile - ls[c] * ups[c]
            tiles[t] = tile
            if (t + 1) * GROUP - 1 > b:
                tile = extra[t]
                for c in range(8):
                    tile = tile - ls[c] * ups2[c]
                extra[t] = tile
    return tuple(jnp.concatenate(x, 0) for x in (packed, lower, tiles))


def lu_step(k, packed, li, ui):
    n = ui.shape[0]
    o = pl.multiple_of(k * 128, 128)
    blk = pl.ds(o, 128)
    own, lower, upper = lu128(ui[blk, blk])
    lower, upper = split(lower), split(upper)
    past = lax.broadcasted_iota(jnp.int32, (128, n), 1) >= o + 128
    diag = lax.broadcasted_iota(jnp.int32, (128, n), 1) == (
        lax.broadcasted_iota(jnp.int32, (128, n), 0) + o
    )
    band = ui[blk, :]
    right = dot3(lower, split(band))
    packed[blk, :] = jnp.where(past, right, band)
    packed[blk, blk] = own
    ui[blk, :] = jnp.where(diag, 1.0, 0.0)
    left = dot3(split(ui[:, blk]), upper)
    ui[...] = ui[...] - dot3(split(left), split(jnp.where(past, right, 0.0)))
    ui[:, blk] = left
    lband = dot3(lower, split(li[blk, :]))
    li[blk, :] = lband
    below = lax.broadcasted_iota(jnp.int32, (n, 128), 0) >= o + 128
    li[...] = li[...] - dot3(split(jnp.where(below, left, 0.0)), split(lband))


def kernel(hbm, rd, cd, o, x, rdo, cds, xin, rs, t, m11, m12, m21, packed, li, ui, mh, ml, uf, wh, wl, lih, lil, uih, uil, z, send, recv, load):
    r, c = lax.axis_index("row"), lax.axis_index("col")
    q, g = c // 16, c % 16
    m = r * 4 + q
    core, pair = g % 2, g // 2

    def member(p):
        return {"row": p // 4, "col": (p % 4) * 16 + g}

    def chip(d):
        return {"row": r, "col": (m % 4) * 16 + (g + 2 * d) % 16}

    partner = {"row": r, "col": (m % 4) * 16 + g + 1 - 2 * core}

    def device(p):
        return {"row": r, "col": (m % 4) * 16 + p}

    def remote(src, dst, kind, out, into, where):
        return pltpu.make_async_remote_copy(
            src, dst, send.at[kind, out], recv.at[kind, into], device_id=where, device_id_type=MESH
        )

    def rows(p, height, base=0):
        return pl.ds(pl.multiple_of(base + height * p, 8), height)

    def head(d):
        p = (m + d) % 8
        return remote(x.at[:, rows(p, 64)], xin.at[m, :, pl.ds(0, 64)], 0, d, d, member(p))

    def small(d):
        if d == 0:
            return remote(rd, rdo, 1, 0, 0, member((m + 4) % 8))
        return remote(cd, cds.at[q], 1, d, d, member(r * 4 + (q + d) % 4))

    def tail(d, unit):
        p = (m + d) % 8
        return remote(
            x.at[:, pl.ds(pl.multiple_of(192 * p + 448 + 64 * unit, 8), 64)],
            xin.at[m, :, pl.ds(64 * unit, 64)],
            (0, 2, 3, 14)[unit],
            d,
            d,
            member(p),
        )

    def top(d):
        return remote(t.at[0, 0, pl.ds(0, 64)], m21.at[0, core, pair], 4, d, pair, chip(d))

    def top_over():
        return remote(m21.at[0, core], m21.at[0, core], 5, 0, 0, partner)

    def corner(d):
        return remote(m21.at[0, core], m11.at[m, core], 6, d, d, member((m + d) % 8))

    def corner_over(d):
        p = (m + 8 - d) % 8
        return remote(m11.at[p, core], m11.at[p, core], 7, d, d, partner)

    def band(d):
        return remote(t.at[pl.ds(0, 4), 0, pl.ds(0, 64)], m12.at[m], 8, d, d, member((m + d) % 8))

    def piece(p):
        return t.at[(p // 8) * 4, (p % 8) // 4, rows(p % 4, 64)]

    def part(p, plane):
        return pltpu.make_async_remote_copy(
            piece(p),
            m21.at[p, core, pair],
            send.at[9 + 6 * plane, p],
            recv.at[9, g + 4 * (p // 8)],
            device_id=device(8 * plane + p % 8),
            device_id_type=MESH,
        )

    def parts(unit):
        @pl.when(g < 4)
        def _():
            for i in range(4):
                p = 4 * i + unit
                if p == 0:
                    continue
                part(p, 1).start()
                if p % 8 >= 4:
                    part(p, 0).start()
                else:

                    @pl.when(g != p % 8)
                    def _():
                        part(p, 0).start()

                    @pl.when(g == p % 8)
                    def _():
                        m21[p, core, pair] = piece(p)[...]

    def spread(unit):
        @pl.when(g % 4 == unit)
        def _():
            for e in range(2):

                @pl.when(here + 8 * e != 0)
                def _():
                    for i in range(4):

                        @pl.when(g != i)
                        def _():
                            remote(
                                piece(here), m21.at[here + 8 * e, i % 2, i // 2], 9, 0, i + 4 * e, partner
                            ).wait_recv()

                    for d in range(1, 4):
                        panel(e, d).start()
                    panel_over(here // 2 + 4 * e).start()

    def arrive(unit):
        for d in range(1, 8):
            tail(d, unit).wait()
        lax.fori_loop(8 * unit, 8 * unit + 8, functools.partial(mix, 64), 0)

    here = g % 8

    def panel(e, d):
        p = here + 8 * e
        where = device(8 * (g // 8) + (here + 2 * d) % 8)
        return remote(m21.at[p], m21.at[p], 10, 4 * e + d, here // 2 + 4 * e, where)

    def panel_over(j):
        p = 2 * j + core
        return remote(m21.at[p], m21.at[p], 11, j, j, partner)

    def target(slot):
        half = slot // 4
        return 4 * ((r + 1 + half) % 2) + (q + slot + half) % 4

    def back(slot, first):
        p = target(slot)
        if first:
            return remote(z.at[p, :, pl.ds(0, 64)], o.at[:, rows(m, 64)], 12, slot, slot, member(p))
        return remote(z.at[p, :, pl.ds(64, 192)], o.at[:, rows(m, 192, 512)], 13, slot, slot, member(p))

    loads = [
        pltpu.make_async_copy(hbm.at[:, pl.ds(0, 512)], x.at[:, pl.ds(0, 512)], load.at[0]),
        pltpu.make_async_copy(hbm.at[:, pl.ds(512, 1536)], x.at[:, pl.ds(512, 1536)], load.at[1]),
    ]
    for copy in loads:
        copy.start()

    bar = pltpu.get_barrier_semaphore()
    for d in range(1, 8):
        pl.semaphore_signal(bar, inc=1, device_id=member((m + d) % 8), device_id_type=MESH)
    for d in range(1, 16):
        pl.semaphore_signal(bar, inc=1, device_id=device((g + d) % 16), device_id_type=MESH)
    pl.semaphore_wait(bar, 22)

    for d in range(4):
        small(d).start()
    loads[0].wait()
    for d in range(1, 8):
        head(d).start()
    cds[q] = cd[...]
    xin[m, :, 0:64] = x[:, rows(m, 64)]
    loads[1].wait()
    for d in EARLY:
        tail(d, 1).start()
    xin[m, :, 64:256] = x[:, rows(m, 192, 512)]

    def widen(source, i):
        for l in range(2):
            for h in range(2):
                for j in range(3):
                    at = 16 * h + (m // 2 if j == 0 else 3 + j + 3 * m // 2)
                    line = source[l : l + 1, pl.ds(pl.multiple_of(128 * at, 128), 128)]
                    rs[l, i, h, 128 * j : 128 * j + 128] = rows_to(line, 128).T

    widen(rd, r)
    for d in range(4):
        small(d).wait()
    widen(rdo, 1 - r)

    def mix(base, j, _):
        at = pl.ds(pl.multiple_of(8 * j, 8), 8)
        to = pl.ds(pl.multiple_of(8 * j + base + 64 * (m % 2), 8), 8)
        first = [rows_to(cds[q, 0:1, :], 8) for q in range(4)]
        second = [rows_to(cds[q, 1:2, :] * 0.25, 8) for q in range(4)]
        for i in range(2):
            mid = {}
            for q in range(4):
                y = []
                for h in range(2):
                    a, b = xin[q, h, at], xin[4 + q, h, at]
                    y.append(rs[0, i, h, to] * (a + b if i == 0 else a - b))
                mid[q] = [rs[1, i, 0, to] * (y[0] + y[1]), rs[1, i, 1, to] * (y[0] - y[1])]
            for h in range(2):
                w = [first[q] * (mid[q][h] + mid[q + 2][h]) for q in range(2)]
                w += [first[q + 2] * (mid[q][h] - mid[q + 2][h]) for q in range(2)]
                for q in (0, 2):
                    t[4 * i + q, h, at] = second[q] * (w[q] + w[q + 1])
                    t[4 * i + q + 1, h, at] = second[q + 1] * (w[q] - w[q + 1])
        return 0

    for d in range(1, 8):
        head(d).wait()
    lax.fori_loop(0, 8, functools.partial(mix, 0), 0)

    @pl.when(g < 4)
    def _():
        for d in range(1, 8):
            top(d).start()
        m21[0, core, pair] = t[0, 0, 0:64]

    parts(0)

    for i in range(2):

        @pl.when(g != 2 * i + core)
        def _():
            remote(t.at[0, 0, pl.ds(0, 64)], m21.at[0, core, i], 4, 0, i, partner).wait_recv()

    for d in range(1, 8):
        corner(d).start()
    top_over().start()
    for d in range(1, 8):
        if d not in EARLY:
            tail(d, 1).start()
    for unit in (2, 3):
        for d in range(1, 8):
            tail(d, unit).start()
    m11[m, core] = m21[0, core]
    m12[m] = t[0:4, 0, 0:64]
    li[...] = jnp.where(
        lax.broadcasted_iota(jnp.int32, li.shape, 0) == lax.broadcasted_iota(jnp.int32, li.shape, 1),
        1.0,
        0.0,
    )
    top_over().wait()
    m11[m, 1 - core] = m21[0, 1 - core]
    for d in range(1, 8):
        corner(d).wait_recv()
        corner_over(d).start()
    for d in range(1, 8):
        corner_over(d).wait()
    for i in range(8):
        for j in range(4):
            ui[64 * i : 64 * i + 64, 128 * j : 128 * j + 128] = m11[i, j % 2, j // 2]

    spread(0)

    def eliminate(k, _):
        lu_step(k, packed, li, ui)

        @pl.when(k == 0)
        def _():
            arrive(1)
            parts(1)
            arrive(2)
            parts(2)
            for d in range(1, 8):
                band(d).start()

        @pl.when(k == 1)
        def _():
            arrive(3)
            parts(3)
            spread(1)
            spread(2)

        @pl.when(k == 2)
        def _():
            spread(3)

        return 0

    lax.fori_loop(0, 4, eliminate, 0)

    def relay(i):
        for k in range(4):
            j = 4 * i + k

            @pl.when((2 * j + core != 0) & (j != here // 2 + 4 * i))
            def _():
                remote(m21.at[here], m21.at[2 * j + core], 10, 0, j, partner).wait_recv()
                panel_over(j).start()

    def left_of(i):
        for k in range(4):
            j = 4 * i + k

            @pl.when(2 * j + 1 - core != 0)
            def _():
                remote(m21.at[here], m21.at[2 * j + 1 - core], 11, 0, j, partner).wait_recv()

        at = pl.ds(8 * i, 8)
        for j in range(4):
            lanes = slice(128 * j, 128 * j + 128)
            mh[i, :, lanes], ml[i, :, lanes] = split(m21[at, j % 2, j // 2].reshape(512, 128))

    own = pl.ds(pl.multiple_of(jnp.minimum(g, 3) * 128, 128), 128)

    def prepare(slot):
        j = (q + slot) % 4
        lanes = pl.ds(pl.multiple_of(128 * j, 128), 128)
        right = dot3((lih[...], lil[...]), split(m12[:, j].reshape(512, 128)))
        uf[:, lanes] = right
        wh[:, lanes], wl[:, lanes] = split(dot3((uih[...], uil[...]), split(right)))

    def finish(slot, _):
        p = target(slot)
        i = p // 4
        lanes = pl.ds(pl.multiple_of(128 * (p % 4), 128), 128)
        got = dot3((mh[i], ml[i]), (wh[:, lanes], wl[:, lanes]))
        z[p] = t[p] - got.reshape(2, 256, 128)

        @pl.when((p % 4 == 0) & (g < 4))
        def _():
            z[p] = dot3((mh[i], ml[i]), (uih[:, own], uil[:, own])).reshape(2, 256, 128)

        @pl.when(i == 0)
        def _():
            z[p, 0, 0:64] = uf[rows(m, 64), lanes]

        @pl.when((p == 0) & (g < 4))
        def _():
            z[p, 0, 0:64] = packed[rows(m, 64), own]

        @pl.when(slot < 7)
        def _():
            back(slot, True).start()
            back(slot, False).start()

        @pl.when(slot < 3)
        def _():
            prepare(slot + 1)

        return 0

    relay(1 - r)
    for d in range(1, 8):
        band(d).wait()
    lih[...], lil[...] = split(li[...])
    uih[...], uil[...] = split(ui[...])
    prepare(0)
    left_of(1 - r)
    relay(r)
    lax.fori_loop(0, 4, finish, 0)
    left_of(r)
    lax.fori_loop(4, 8, finish, 0)
    o[:, rows(m, 64)] = z[m, :, 0:64]
    o[:, rows(m, 192, 512)] = z[m, :, 64:256]

    for d in range(1, 8):
        corner(d).wait_send()

    @pl.when(g < 4)
    def _():
        for d in range(1, 8):
            top(d).wait_send()
        for p in range(1, 16):
            part(p, 1).wait_send()

            @pl.when(g != p % 8)
            def _():
                part(p, 0).wait_send()

    for e in range(2):

        @pl.when(here + 8 * e != 0)
        def _():
            for d in range(1, 4):
                panel(e, d).wait_send()

    for j in range(8):

        @pl.when(2 * j + core != 0)
        def _():
            panel_over(j).wait_send()

    for slot in range(7):
        back(slot, True).wait()
        back(slot, False).wait()


def shards(matrix, row_diag, col_diag):
    f32, bf16 = jnp.float32, jnp.bfloat16
    shapes = [
        ((2, 2048, 128), f32),
        ((2, 4096), f32),
        ((4, 2, 128), f32),
        ((8, 2, 256, 128), f32),
        ((2, 2, 2, 384, 128), f32),
        ((8, 2, 256, 128), f32),
        ((8, 2, 2, 64, 128), f32),
        ((8, 4, 64, 128), f32),
        ((16, 2, 2, 64, 128), f32),
        ((512, 512), f32),
        ((512, 512), f32),
        ((512, 512), f32),
        ((2, 512, 512), bf16),
        ((2, 512, 512), bf16),
        ((512, 512), f32),
        ((512, 512), bf16),
        ((512, 512), bf16),
        ((512, 512), bf16),
        ((512, 512), bf16),
        ((512, 512), bf16),
        ((512, 512), bf16),
        ((8, 2, 256, 128), f32),
    ]
    out = pl.pallas_call(
        kernel,
        out_shape=pltpu.VMEM((2, 2048, 128), f32),
        in_specs=[pl.BlockSpec(memory_space=pl.ANY), VMEM, VMEM],
        out_specs=VMEM,
        scratch_shapes=[pltpu.VMEM(*shape) for shape in shapes]
        + [pltpu.SemaphoreType.DMA((16, 16))] * 2
        + [pltpu.SemaphoreType.DMA((2,))],
        compiler_params=pltpu.CompilerParams(collective_id=0, has_side_effects=True),
        name="whole",
    )(matrix.reshape(2, 2048, 128), row_diag, col_diag)
    return out.reshape(4096, 128)


def solution(mesh):
    in_specs = (P("row", "col"), P(None, "row"), P(None, "col"))
    out_specs = P("row", "col")
    return jax.shard_map(shards, mesh=mesh, in_specs=in_specs, out_specs=out_specs, check_vma=False)
```

```python
import functools

import jax
import jax.numpy as jnp
from jax import lax
from jax.experimental import pallas as pl
from jax.experimental.pallas import tpu as pltpu
from jax.sharding import PartitionSpec as P

MESH = pl.DeviceIdType.MESH
VMEM = pl.BlockSpec(memory_space=pltpu.VMEM)
GROUP = 4
EARLY = (1, 2, 3, 4, 5, 6, 7)


def split(a):
    high = a.astype(jnp.bfloat16)
    return high, (a - high.astype(jnp.float32)).astype(jnp.bfloat16)


def dot(a, b):
    return jnp.dot(a, b, preferred_element_type=jnp.float32)


def dot3(a, b):
    return dot(a[0], b[0]) + (dot(a[0], b[1]) + dot(a[1], b[0]))


def rows_to(x, height):
    return jnp.broadcast_to(x, (height, x.shape[1]))


def lane_to(x, lane):
    return jnp.broadcast_to(x[:, lane : lane + 1], (x.shape[0], 128))


def lu128(s):
    height = 8 * GROUP
    sub = lax.broadcasted_iota(jnp.int32, (8, 128), 0)
    lane = lax.broadcasted_iota(jnp.int32, (8, 128), 1)
    subs = lax.broadcasted_iota(jnp.int32, (height, 128), 0)
    lanes = lax.broadcasted_iota(jnp.int32, (height, 128), 1)
    count = 16 // GROUP
    tiles = [s[height * t : height * t + height] for t in range(count)]
    extra = [jnp.where(lanes == subs + height * t, 1.0, 0.0) for t in range(count)]
    packed, lower = [], []

    def tall(x):
        return jnp.concatenate([x] * GROUP, 0)

    for b in range(16):
        at, part = b // GROUP, 8 * (b % GROUP)
        rows, rows2 = tiles[at][part : part + 8], extra[at][part : part + 8]
        cols = [lane_to(rows, 8 * b + c) for c in range(8)]
        inner = (lane >= 8 * b) & (lane < 8 * b + 8)
        full = jnp.where(lane >= 8 * b + 8, rows, jnp.where(lane == sub + 8 * b, -1.0, 0.0))
        full2 = rows2
        for c in range(8):
            column = cols[c]
            r = 1.0 / rows_to(column[c : c + 1], 8)
            factor = jnp.where(sub > c, column * r, 0.0)
            for d in range(c + 1, 8):
                row = rows_to(cols[d][c : c + 1], 8) * r
                cols[d] = jnp.where(sub == c, row, cols[d] - column * row)
            row = rows_to(full[c : c + 1], 8) * r
            full = jnp.where(sub == c, row, full - jnp.where(inner & (sub > c), 0.0, column) * row)
            row = rows_to(full2[c : c + 1], 8) * r
            full2 = jnp.where(sub == c, row, full2 - column * row)
            top = jnp.where(lane > 8 * b + c, rows_to(rows[c : c + 1], 8), 0.0)
            rows = jnp.where((lane == 8 * b + c) & (sub > c), factor, rows - factor * top)
            if c < 7:
                rows2 = rows2 - factor * rows_to(rows2[c : c + 1], 8)
        packed.append(rows)
        lower.append(rows2)
        pieces = [jnp.where(lane == sub + 8 * b, 1.0, 0.0)]
        if part:
            pieces = [tiles[at][:part]] + pieces
        if part + 8 < height:
            pieces = pieces + [tiles[at][part + 8 :]]
        tiles[at] = jnp.concatenate(pieces, 0) if len(pieces) > 1 else pieces[0]
        inside = (lanes >= 8 * b) & (lanes < 8 * b + 8)
        ups = [tall(rows_to(full[c : c + 1], 8)) for c in range(8)]
        ups2 = [tall(rows_to(full2[c : c + 1], 8)) for c in range(8)]
        for i in range(count):
            t = ((b + 1) // GROUP + i) % count
            tile = tiles[t]
            ls = [lane_to(tile, 8 * b + c) for c in range(8)]
            tile = jnp.where(inside, 0.0, tile)
            for c in range(8):
                tile = tile - ls[c] * ups[c]
            tiles[t] = tile
            if (t + 1) * GROUP - 1 > b:
                tile = extra[t]
                for c in range(8):
                    tile = tile - ls[c] * ups2[c]
                extra[t] = tile
    return tuple(jnp.concatenate(x, 0) for x in (packed, lower, tiles))


def lu_step(k, packed, li, ui):
    n = ui.shape[0]
    o = pl.multiple_of(k * 128, 128)
    blk = pl.ds(o, 128)
    own, lower, upper = lu128(ui[blk, blk])
    lower, upper = split(lower), split(upper)
    past = lax.broadcasted_iota(jnp.int32, (128, n), 1) >= o + 128
    diag = lax.broadcasted_iota(jnp.int32, (128, n), 1) == (
        lax.broadcasted_iota(jnp.int32, (128, n), 0) + o
    )
    band = ui[blk, :]
    right = dot3(lower, split(band))
    packed[blk, :] = jnp.where(past, right, band)
    packed[blk, blk] = own
    ui[blk, :] = jnp.where(diag, 1.0, 0.0)
    left = dot3(split(ui[:, blk]), upper)
    ui[...] = ui[...] - dot3(split(left), split(jnp.where(past, right, 0.0)))
    ui[:, blk] = left
    lband = dot3(lower, split(li[blk, :]))
    li[blk, :] = lband
    below = lax.broadcasted_iota(jnp.int32, (n, 128), 0) >= o + 128
    li[...] = li[...] - dot3(split(jnp.where(below, left, 0.0)), split(lband))


def kernel(hbm, rd, cd, o, x, rdo, cds, xin, rs, t, m11, m12, m21, packed, li, ui, mh, ml, uf, wh, wl, lih, lil, uih, uil, z, send, recv, load):
    r, c = lax.axis_index("row"), lax.axis_index("col")
    q, g = c // 16, c % 16
    m = r * 4 + q
    core, pair = g % 2, g // 2

    def member(p):
        return {"row": p // 4, "col": (p % 4) * 16 + g}

    def chip(d):
        return {"row": r, "col": (m % 4) * 16 + (g + 2 * d) % 16}

    partner = {"row": r, "col": (m % 4) * 16 + g + 1 - 2 * core}

    def device(p):
        return {"row": r, "col": (m % 4) * 16 + p}

    def remote(src, dst, kind, out, into, where):
        return pltpu.make_async_remote_copy(
            src, dst, send.at[kind, out], recv.at[kind, into], device_id=where, device_id_type=MESH
        )

    def rows(p, height, base=0):
        return pl.ds(pl.multiple_of(base + height * p, 8), height)

    def head(d):
        p = (m + d) % 8
        return remote(x.at[:, rows(p, 64)], xin.at[m, :, pl.ds(0, 64)], 0, d, d, member(p))

    def small(d):
        if d == 0:
            return remote(rd, rdo, 1, 0, 0, member((m + 4) % 8))
        return remote(cd, cds.at[q], 1, d, d, member(r * 4 + (q + d) % 4))

    def tail(d, unit):
        p = (m + d) % 8
        return remote(
            x.at[:, pl.ds(pl.multiple_of(192 * p + 448 + 64 * unit, 8), 64)],
            xin.at[m, :, pl.ds(64 * unit, 64)],
            (0, 2, 3, 14)[unit],
            d,
            d,
            member(p),
        )

    def top(d):
        return remote(t.at[0, 0, pl.ds(0, 64)], m21.at[0, core, pair], 4, d, pair, chip(d))

    def top_over():
        return remote(m21.at[0, core], m21.at[0, core], 5, 0, 0, partner)

    def corner(d):
        return remote(m21.at[0, core], m11.at[m, core], 6, d, d, member((m + d) % 8))

    def corner_over(d):
        p = (m + 8 - d) % 8
        return remote(m11.at[p, core], m11.at[p, core], 7, d, d, partner)

    def band(d):
        return remote(t.at[pl.ds(0, 4), 0, pl.ds(0, 64)], m12.at[m], 8, d, d, member((m + d) % 8))

    def piece(p):
        return t.at[(p // 8) * 4, (p % 8) // 4, rows(p % 4, 64)]

    def part(p, plane):
        return pltpu.make_async_remote_copy(
            piece(p),
            m21.at[p, core, pair],
            send.at[9 + 6 * plane, p],
            recv.at[9, g + 4 * (p // 8)],
            device_id=device(8 * plane + p % 8),
            device_id_type=MESH,
        )

    def parts(unit):
        @pl.when(g < 4)
        def _():
            for i in range(4):
                p = 4 * i + unit
                if p == 0:
                    continue
                part(p, 1).start()
                if p % 8 >= 4:
                    part(p, 0).start()
                else:

                    @pl.when(g != p % 8)
                    def _():
                        part(p, 0).start()

                    @pl.when(g == p % 8)
                    def _():
                        m21[p, core, pair] = piece(p)[...]

    def spread(unit):
        @pl.when(g % 4 == unit)
        def _():
            for e in range(2):

                @pl.when(here + 8 * e != 0)
                def _():
                    for i in range(4):

                        @pl.when(g != i)
                        def _():
                            remote(
                                piece(here), m21.at[here + 8 * e, i % 2, i // 2], 9, 0, i + 4 * e, partner
                            ).wait_recv()

                    for d in range(1, 4):
                        panel(e, d).start()
                    panel_over(here // 2 + 4 * e).start()

    def arrive(unit):
        for d in range(1, 8):
            tail(d, unit).wait()
        lax.fori_loop(8 * unit, 8 * unit + 8, functools.partial(mix, 64), 0)

    here = g % 8

    def panel(e, d):
        p = here + 8 * e
        where = device(8 * (g // 8) + (here + 2 * d) % 8)
        return remote(m21.at[p], m21.at[p], 10, 4 * e + d, here // 2 + 4 * e, where)

    def panel_over(j):
        p = 2 * j + core
        return remote(m21.at[p], m21.at[p], 11, j, j, partner)

    def target(slot):
        half = slot % 2
        return 4 * ((r + 1 + half) % 2) + (q + (slot + 1) // 2) % 4

    def back(slot, first):
        p = target(slot)
        if first:
            return remote(z.at[p, :, pl.ds(0, 64)], o.at[:, rows(m, 64)], 12, slot, slot, member(p))
        return remote(z.at[p, :, pl.ds(64, 192)], o.at[:, rows(m, 192, 512)], 13, slot, slot, member(p))

    loads = [
        pltpu.make_async_copy(hbm.at[:, pl.ds(0, 512)], x.at[:, pl.ds(0, 512)], load.at[0]),
        pltpu.make_async_copy(hbm.at[:, pl.ds(512, 1536)], x.at[:, pl.ds(512, 1536)], load.at[1]),
    ]
    for copy in loads:
        copy.start()

    bar = pltpu.get_barrier_semaphore()
    for d in range(1, 8):
        pl.semaphore_signal(bar, inc=1, device_id=member((m + d) % 8), device_id_type=MESH)
    for d in range(1, 16):
        pl.semaphore_signal(bar, inc=1, device_id=device((g + d) % 16), device_id_type=MESH)
    pl.semaphore_wait(bar, 22)

    for d in range(4):
        small(d).start()
    loads[0].wait()
    for d in range(1, 8):
        head(d).start()
    cds[q] = cd[...]
    xin[m, :, 0:64] = x[:, rows(m, 64)]
    loads[1].wait()
    for d in EARLY:
        tail(d, 1).start()
    xin[m, :, 64:256] = x[:, rows(m, 192, 512)]

    def widen(source, i):
        for l in range(2):
            for h in range(2):
                for j in range(3):
                    at = 16 * h + (m // 2 if j == 0 else 3 + j + 3 * m // 2)
                    line = source[l : l + 1, pl.ds(pl.multiple_of(128 * at, 128), 128)]
                    rs[l, i, h, 128 * j : 128 * j + 128] = rows_to(line, 128).T

    widen(rd, r)
    for d in range(4):
        small(d).wait()
    widen(rdo, 1 - r)

    def mix(base, j, _):
        at = pl.ds(pl.multiple_of(8 * j, 8), 8)
        to = pl.ds(pl.multiple_of(8 * j + base + 64 * (m % 2), 8), 8)
        first = [rows_to(cds[q, 0:1, :], 8) for q in range(4)]
        second = [rows_to(cds[q, 1:2, :] * 0.25, 8) for q in range(4)]
        for i in range(2):
            mid = {}
            for q in range(4):
                y = []
                for h in range(2):
                    a, b = xin[q, h, at], xin[4 + q, h, at]
                    y.append(rs[0, i, h, to] * (a + b if i == 0 else a - b))
                mid[q] = [rs[1, i, 0, to] * (y[0] + y[1]), rs[1, i, 1, to] * (y[0] - y[1])]
            for h in range(2):
                w = [first[q] * (mid[q][h] + mid[q + 2][h]) for q in range(2)]
                w += [first[q + 2] * (mid[q][h] - mid[q + 2][h]) for q in range(2)]
                for q in (0, 2):
                    t[4 * i + q, h, at] = second[q] * (w[q] + w[q + 1])
                    t[4 * i + q + 1, h, at] = second[q + 1] * (w[q] - w[q + 1])
        return 0

    for d in range(1, 8):
        head(d).wait()
    lax.fori_loop(0, 8, functools.partial(mix, 0), 0)

    @pl.when(g < 4)
    def _():
        for d in range(1, 8):
            top(d).start()
        m21[0, core, pair] = t[0, 0, 0:64]

    parts(0)

    for i in range(2):

        @pl.when(g != 2 * i + core)
        def _():
            remote(t.at[0, 0, pl.ds(0, 64)], m21.at[0, core, i], 4, 0, i, partner).wait_recv()

    for d in range(1, 8):
        corner(d).start()
    top_over().start()
    for d in range(1, 8):
        if d not in EARLY:
            tail(d, 1).start()
    for unit in (2, 3):
        for d in range(1, 8):
            tail(d, unit).start()
    m11[m, core] = m21[0, core]
    m12[m] = t[0:4, 0, 0:64]
    li[...] = jnp.where(
        lax.broadcasted_iota(jnp.int32, li.shape, 0) == lax.broadcasted_iota(jnp.int32, li.shape, 1),
        1.0,
        0.0,
    )
    top_over().wait()
    m11[m, 1 - core] = m21[0, 1 - core]
    for d in range(1, 8):
        corner(d).wait_recv()
        corner_over(d).start()
    for d in range(1, 8):
        corner_over(d).wait()
    for i in range(8):
        for j in range(4):
            ui[64 * i : 64 * i + 64, 128 * j : 128 * j + 128] = m11[i, j % 2, j // 2]

    spread(0)

    def eliminate(k, _):
        lu_step(k, packed, li, ui)

        @pl.when(k == 0)
        def _():
            arrive(1)
            parts(1)
            arrive(2)
            parts(2)
            for d in range(1, 8):
                band(d).start()

        @pl.when(k == 1)
        def _():
            arrive(3)
            parts(3)
            spread(1)
            spread(2)

        @pl.when(k == 2)
        def _():
            spread(3)

        return 0

    lax.fori_loop(0, 4, eliminate, 0)

    def relay(i):
        for k in range(4):
            j = 4 * i + k

            @pl.when((2 * j + core != 0) & (j != here // 2 + 4 * i))
            def _():
                remote(m21.at[here], m21.at[2 * j + core], 10, 0, j, partner).wait_recv()
                panel_over(j).start()

    def left_of(i):
        for k in range(4):
            j = 4 * i + k

            @pl.when(2 * j + 1 - core != 0)
            def _():
                remote(m21.at[here], m21.at[2 * j + 1 - core], 11, 0, j, partner).wait_recv()

        at = pl.ds(8 * i, 8)
        for j in range(4):
            lanes = slice(128 * j, 128 * j + 128)
            mh[i, :, lanes], ml[i, :, lanes] = split(m21[at, j % 2, j // 2].reshape(512, 128))

    own = pl.ds(pl.multiple_of(jnp.minimum(g, 3) * 128, 128), 128)

    def prepare(slot):
        j = (q + slot) % 4
        lanes = pl.ds(pl.multiple_of(128 * j, 128), 128)
        right = dot3((lih[...], lil[...]), split(m12[:, j].reshape(512, 128)))
        uf[:, lanes] = right
        wh[:, lanes], wl[:, lanes] = split(dot3((uih[...], uil[...]), split(right)))

    def finish(slot, _):
        p = target(slot)
        i = p // 4
        lanes = pl.ds(pl.multiple_of(128 * (p % 4), 128), 128)
        got = dot3((mh[i], ml[i]), (wh[:, lanes], wl[:, lanes]))
        z[p] = t[p] - got.reshape(2, 256, 128)

        @pl.when((p % 4 == 0) & (g < 4))
        def _():
            z[p] = dot3((mh[i], ml[i]), (uih[:, own], uil[:, own])).reshape(2, 256, 128)

        @pl.when(i == 0)
        def _():
            z[p, 0, 0:64] = uf[rows(m, 64), lanes]

        @pl.when((p == 0) & (g < 4))
        def _():
            z[p, 0, 0:64] = packed[rows(m, 64), own]

        @pl.when(slot < 7)
        def _():
            back(slot, True).start()
            back(slot, False).start()

        @pl.when((slot < 5) & (slot % 2 == 0))
        def _():
            prepare(slot // 2 + 1)

        return 0

    relay(1 - r)
    relay(r)
    for d in range(1, 8):
        band(d).wait()
    lih[...], lil[...] = split(li[...])
    uih[...], uil[...] = split(ui[...])
    prepare(0)
    left_of(1 - r)
    left_of(r)
    lax.fori_loop(0, 8, finish, 0)
    o[:, rows(m, 64)] = z[m, :, 0:64]
    o[:, rows(m, 192, 512)] = z[m, :, 64:256]

    for d in range(1, 8):
        corner(d).wait_send()

    @pl.when(g < 4)
    def _():
        for d in range(1, 8):
            top(d).wait_send()
        for p in range(1, 16):
            part(p, 1).wait_send()

            @pl.when(g != p % 8)
            def _():
                part(p, 0).wait_send()

    for e in range(2):

        @pl.when(here + 8 * e != 0)
        def _():
            for d in range(1, 4):
                panel(e, d).wait_send()

    for j in range(8):

        @pl.when(2 * j + core != 0)
        def _():
            panel_over(j).wait_send()

    for slot in range(7):
        back(slot, True).wait()
        back(slot, False).wait()


def shards(matrix, row_diag, col_diag):
    f32, bf16 = jnp.float32, jnp.bfloat16
    shapes = [
        ((2, 2048, 128), f32),
        ((2, 4096), f32),
        ((4, 2, 128), f32),
        ((8, 2, 256, 128), f32),
        ((2, 2, 2, 384, 128), f32),
        ((8, 2, 256, 128), f32),
        ((8, 2, 2, 64, 128), f32),
        ((8, 4, 64, 128), f32),
        ((16, 2, 2, 64, 128), f32),
        ((512, 512), f32),
        ((512, 512), f32),
        ((512, 512), f32),
        ((2, 512, 512), bf16),
        ((2, 512, 512), bf16),
        ((512, 512), f32),
        ((512, 512), bf16),
        ((512, 512), bf16),
        ((512, 512), bf16),
        ((512, 512), bf16),
        ((512, 512), bf16),
        ((512, 512), bf16),
        ((8, 2, 256, 128), f32),
    ]
    out = pl.pallas_call(
        kernel,
        out_shape=pltpu.VMEM((2, 2048, 128), f32),
        in_specs=[pl.BlockSpec(memory_space=pl.ANY), VMEM, VMEM],
        out_specs=VMEM,
        scratch_shapes=[pltpu.VMEM(*shape) for shape in shapes]
        + [pltpu.SemaphoreType.DMA((16, 16))] * 2
        + [pltpu.SemaphoreType.DMA((2,))],
        compiler_params=pltpu.CompilerParams(collective_id=0, has_side_effects=True),
        name="whole",
    )(matrix.reshape(2, 2048, 128), row_diag, col_diag)
    return out.reshape(4096, 128)


def solution(mesh):
    in_specs = (P("row", "col"), P(None, "row"), P(None, "col"))
    out_specs = P("row", "col")
    return jax.shard_map(shards, mesh=mesh, in_specs=in_specs, out_specs=out_specs, check_vma=False)
```
